32 devices in a mesh: tm: 8 (over z, y), space: 4 (over x, core).
Axes of the slice: x: 2, y: 2, z: 4, core: 2. Of those that a mesh axis runs over, the one named last changes fastest.
Arguments:
- initial: float32 [8, 128, 128], P('space'), may hold values from -6 to 6
- start_guess: float32 [8, 8, 128, 128], P('tm', 'space'), may hold values from -6 to 6
- forcing: float32 [8, 5, 8, 128, 128], P('tm', None, 'space'), may hold values from -6 to 6
- step_size: float32 [8], P('tm'), may hold values from 0.06 to 0.16
Outputs:
- fine_values: float32 [8, 5, 8, 128, 128], P('tm', None, 'space')
The draws below stay inside these ranges and needn't reach their ends.
All inputs are finite; a program needn't handle non-finite values.
Results may differ from the reference program's by a relative error of at most 0.0001.
Values sent between devices are 32-bit elements; how exact they have to be, the bound alone decides.
No kernel may reach another device: no remote copies, remote signals or barrier semaphores. Data moves between devices by JAX's collectives and lax.ppermute only.
A program may use at most 64 MiB of HBM per device.

```python
import math
import jax
import jax.numpy as jnp
import numpy as np
from jax import lax

NX = 128
NY = 128
NODES = 5
ITERS = 2
NTIME = 8
NZ = 8


def level_of(rng, shape, cuts, low, top_value):
    gain, own = 1.0, jax.random.fold_in(rng, 6)
    for axis_at, blocks in cuts:
        steps = jnp.exp(jax.random.uniform(jax.random.fold_in(own, axis_at), (blocks,), jnp.float32, low / len(cuts), top_value / len(cuts)))
        gain = gain * jnp.repeat(steps, shape[axis_at] // blocks).reshape([-1 if axis == axis_at else 1 for axis in range(len(shape))])
    return gain


def centred(stream_key, shape, scale, bound, shards=(), kind=jnp.bfloat16):
    result = scale * jax.random.normal(stream_key, shape, jnp.float32)
    if shards:
        result = result * level_of(stream_key, shape, shards, -0.22, 0.18)
    return jnp.clip(result, -bound, bound).astype(kind)


def setup_inputs(seed: int = 0) -> dict:
    arg_keys = jax.random.split(jax.random.key(seed), 5)
    return {
        "initial": centred(arg_keys[0], (NZ, NX, NY), 1.0, 6.0, ((0, 4),), jnp.float32),
        "start_guess": centred(arg_keys[1], (NTIME, NZ, NX, NY), 1.0, 6.0, ((0, 8), (1, 4)), jnp.float32),
        "forcing": centred(arg_keys[2], (NTIME, NODES, NZ, NX, NY), 1.0, 6.0, ((0, 8), (2, 4)), jnp.float32),
        "step_size": jnp.clip(jnp.exp(math.log(0.16) - 0.98082925 * jax.random.uniform(arg_keys[3], (NTIME,), jnp.float32) ** level_of(arg_keys[3], (NTIME,), ((0, 8),), -0.2, 0.2)), 0.06, 0.16),
    }


def node_tables():
    radical = math.sqrt(3.0 / 7.0)
    node_times = [0.0, (1.0 - radical) / 2.0, 0.5, (1.0 + radical) / 2.0, 1.0]
    integrals = np.zeros((4, 5))
    for column in range(5):
        coeffs = [1.0]
        for other_index in range(5):
            if other_index == column:
                continue
            other_time = node_times[other_index]
            scaling = node_times[column] - other_time
            grown = [0.0] * (len(coeffs) + 1)
            for exponent in range(len(coeffs)):
                grown[exponent + 1] += coeffs[exponent] / scaling
                grown[exponent] -= coeffs[exponent] * other_time / scaling
            coeffs = grown
        for section in range(4):
            integrals[section, column] = sum((coeffs[exponent] * (node_times[section + 1] ** (exponent + 1) - node_times[section] ** (exponent + 1)) / (exponent + 1) for exponent in range(len(coeffs))))
    coarse = [0.0, 0.5, 1.0]
    interp = np.zeros((5, 3))
    for column in range(3):
        for section in range(5):
            weight = 1.0
            for other_index in range(3):
                if other_index != column:
                    weight = weight * (node_times[section] - coarse[other_index]) / (coarse[column] - coarse[other_index])
            interp[section, column] = weight
    return (np.array(node_times), integrals, interp)

def laplace(field):
    widths = [(0, 0)] * (field.ndim - 3) + [(1, 1)] * 3
    padded = jnp.pad(field, widths)
    center = padded[..., 1:-1, 1:-1, 1:-1]
    return padded[..., 2:, 1:-1, 1:-1] + padded[..., :-2, 1:-1, 1:-1] + padded[..., 1:-1, 2:, 1:-1] + padded[..., 1:-1, :-2, 1:-1] + padded[..., 1:-1, 1:-1, 2:] + padded[..., 1:-1, 1:-1, :-2] - 6.0 * center

def fine_sweep(values, forcing, full_step, node_times, integrals):
    half_step = 0.5 * full_step
    lap_old = laplace(values)
    rates = lap_old + forcing
    swept = [values[0]]
    lap_new = [lap_old[0]]
    for section in range(4):
        quadrature = sum((float(integrals[section, column]) * rates[column] for column in range(5)))
        spacing = float(node_times[section + 1] - node_times[section])
        advanced = swept[section] + full_step * spacing * (lap_new[section] - lap_old[section]) + full_step * quadrature
        swept.append(advanced)
        lap_new.append(laplace(advanced))
    new_rates = [lap_new[column] + forcing[column] for column in range(5)]
    first_half = full_step * sum((float(integrals[0, column] + integrals[1, column]) * new_rates[column] for column in range(5)))
    second_half = full_step * sum((float(integrals[2, column] + integrals[3, column]) * new_rates[column] for column in range(5)))
    left = first_half - half_step * lap_new[0]
    right = second_half - half_step * lap_new[2]
    return (jnp.stack(swept), left, right)

def reference(initial, start_guess, forcing, step_size):
    node_times, integrals, interp = node_tables()
    values = jnp.broadcast_to(start_guess[:, None], (NTIME, NODES, NZ, NX, NY))

    def link(start_value, packed):
        left_term, right_term, half_step = packed
        middle = start_value + half_step * laplace(start_value) + left_term
        ending = middle + half_step * laplace(middle) + right_term
        return (ending, (start_value, middle, ending))
    for sweep_round in range(ITERS):
        starts = jnp.concatenate([initial[None], values[:-1, NODES - 1]], axis=0)
        values = values.at[:, 0].set(starts)
        swept, left, right = lax.map(lambda packed: fine_sweep(packed[0], packed[1], packed[2], node_times, integrals), (values, forcing, step_size))
        last_value, coarse = lax.scan(link, initial, (left, right, 0.5 * step_size))
        deltas = [coarse[0] - swept[:, 0], coarse[1] - swept[:, 2], coarse[2] - swept[:, 4]]
        values = jnp.stack([swept[:, section] + sum((float(interp[section, column]) * deltas[column] for column in range(3))) for section in range(5)], axis=1)
    return values
```

```python
import functools
import math

import jax
import jax.numpy as jnp
import numpy as np
from jax import lax
from jax.experimental import pallas as pl
from jax.experimental.pallas import tpu as pltpu
from jax.sharding import Mesh
from jax.sharding import PartitionSpec as P

TILE = 8


def node_tables():
    radical = math.sqrt(3.0 / 7.0)
    node_times = [0.0, (1.0 - radical) / 2.0, 0.5, (1.0 + radical) / 2.0, 1.0]
    integrals = np.zeros((4, 5))
    for column in range(5):
        coeffs = [1.0]
        for other_index in range(5):
            if other_index == column:
                continue
            other_time = node_times[other_index]
            scaling = node_times[column] - other_time
            grown = [0.0] * (len(coeffs) + 1)
            for exponent in range(len(coeffs)):
                grown[exponent + 1] += coeffs[exponent] / scaling
                grown[exponent] -= coeffs[exponent] * other_time / scaling
            coeffs = grown
        for section in range(4):
            integrals[section, column] = sum(
                coeffs[exponent]
                * (node_times[section + 1] ** (exponent + 1) - node_times[section] ** (exponent + 1))
                / (exponent + 1)
                for exponent in range(len(coeffs))
            )
    coarse = [0.0, 0.5, 1.0]
    interp = np.zeros((5, 3))
    for column in range(3):
        for section in range(5):
            weight = 1.0
            for other_index in range(3):
                if other_index != column:
                    weight = (
                        weight
                        * (node_times[section] - coarse[other_index])
                        / (coarse[column] - coarse[other_index])
                    )
            interp[section, column] = weight
    return (np.array(node_times), integrals, interp)


TIMES, QUAD, INTERP = node_tables()
SPACING = np.diff(TIMES)
LEFT = QUAD[0] + QUAD[1]
RIGHT = QUAD[2] + QUAD[3]


def sine(length):
    index = np.arange(1, length + 1)
    return math.sqrt(2.0 / (length + 1)) * np.sin(math.pi / (length + 1) * np.outer(index, index))


def eigen(length):
    return 2.0 - 2.0 * np.cos(math.pi / (length + 1) * np.arange(1, length + 1))


def halves(matrix):
    high = matrix.astype(jnp.bfloat16).astype(np.float64)
    return high, matrix - high


def right_table(length):
    high, low = halves(sine(length))
    return np.block([[high, low], [high, np.zeros_like(high)]]).astype(jnp.bfloat16)


def left_table(length):
    high, low = halves(sine(length))
    return np.block([[high, high], [low, np.zeros_like(high)]]).astype(jnp.bfloat16)


def split(value):
    high = value.astype(jnp.bfloat16)
    return high, (value - high.astype(jnp.float32)).astype(jnp.bfloat16)


def times_sine(value, table):
    width = value.shape[-1]
    both = jnp.dot(
        jnp.concatenate(split(value), axis=1), table, preferred_element_type=jnp.float32
    )
    return both[:, :width] + both[:, width:]


def sine_times(value, table):
    width = value.shape[0]
    both = jnp.dot(
        table, jnp.concatenate(split(value), axis=0), preferred_element_type=jnp.float32
    )
    return both[:width] + both[width:]


def sine_list(values):
    count = len(values)
    matrix = sine(count)
    half = count // 2
    even = [values[i] + values[count - 1 - i] for i in range(half)]
    odd = [values[i] - values[count - 1 - i] for i in range(half)]
    middle = [values[half]] if count % 2 else []
    result = []
    for k in range(count):
        terms = even + middle if k % 2 == 0 else odd
        result.append(sum(float(matrix[k, i]) * term for i, term in enumerate(terms)))
    return result


def combine(weights, values):
    return sum(float(w) * v for w, v in zip(weights, values) if w != 0.0)


def sweep(first, nodes, forced, scaled):
    swept = [first]
    for m in range(4):
        inner = combine(QUAD[m], nodes)
        if m:
            inner = inner + float(SPACING[m]) * (swept[m] - nodes[m])
        swept.append(swept[m] + (scaled * inner + forced[m]))
    left = scaled * (combine(LEFT, swept) - 0.5 * swept[0]) + (forced[0] + forced[1])
    right = scaled * (combine(RIGHT, swept) - 0.5 * swept[2]) + (forced[2] + forced[3])
    return swept, left, right


def chain(start, left, right, gain):
    middle = gain * start + left
    return middle, gain * middle + right


def correct(swept, start, middle, ending):
    deltas = [start - swept[0], middle - swept[2], ending - swept[4]]
    return [
        start,
        swept[1] + combine(INTERP[1], deltas),
        middle,
        swept[3] + combine(INTERP[3], deltas),
        ending,
    ]


def march(guesses, forced, scaled, state, final):
    before, first, second = state
    fields = []
    for j, guess in enumerate(guesses):
        gain = 1.0 + 0.5 * scaled[j]
        swept, left, right = sweep(before, [before] + [guess] * 4, forced[j], scaled[j])
        middle, ending = chain(first, left, right, gain)
        nodes = correct(swept, first, middle, ending)
        swept, left, right = sweep(first, nodes, forced[j], scaled[j])
        middle, last = chain(second, left, right, gain)
        if final:
            fields.append(correct(swept, second, middle, last))
        before, first, second = guess, ending, last
    return fields if final else (before, first, second)


def forward_kernel(dims, step_ref, init_ref, guess_ref, forcing_ref, right_ref, left_ref, out_ref):
    depth, groups, per, lo, pieces = dims
    step = step_ref[0]
    width = init_ref.shape[1]
    planes = []
    for d in range(depth):
        planes.append(init_ref[d])
        planes.append(guess_ref[0, d])
        samples = [forcing_ref[0, j, d] for j in range(5)]
        for m in range(4):
            planes.append(step * combine(QUAD[m], samples))
    mixed = times_sine(jnp.concatenate(planes, axis=0), right_ref[...])
    mixed = [mixed[i * width : (i + 1) * width] for i in range(len(planes))]
    spectral = []
    for i in range(0, len(mixed), 2):
        pair = sine_times(jnp.concatenate(mixed[i : i + 2], axis=1), left_ref[...])
        spectral += [pair[:, : pair.shape[1] // 2], pair[:, pair.shape[1] // 2 :]]
    fields = 5
    per_plane = len(planes) // depth
    for d in range(depth):
        for f in range(fields):
            row = (f * depth + d) * per
            out_ref[:, row : row + per, :] = spectral[d * per_plane + 1 + f].reshape(
                groups, per, -1
            )
    mine = lax.axis_index("lo")
    rows = per // pieces
    share = None
    for i in range(lo):
        tile = spectral[(i // pieces) * per_plane].reshape(groups, per, -1)
        offset = (i % pieces) * rows
        tile = tile[:, offset : offset + rows]
        share = tile if share is None else jnp.where(mine == i, tile, share)
    base = fields * depth * per
    out_ref[:, base : base + rows, :] = share
    out_ref[:, base + rows :, :] = jnp.full(
        (groups, out_ref.shape[1] - base - rows, out_ref.shape[2]), step, jnp.float32
    )


def owner_weights(dims, space, x_ref, y_ref):
    depth, groups, per, lo, pieces = dims
    owner = lax.axis_index("lo") * space + lax.axis_index("space")
    return x_ref[pl.ds(owner * per, per), :] + y_ref[...]


def gather_kernel(dims, space, got_ref, x_ref, y_ref, modes_ref, start_ref, state_ref):
    depth, groups, per, lo, pieces = dims
    count = depth * space
    base = 5 * depth * per
    rows = per // pieces
    for j in range(lo):
        for f in range(5):
            tiles = []
            for z in range(count):
                row = (f * depth + z % depth) * per
                tiles.append(got_ref[j * space + z // depth, row : row + per, :])
            for z, tile in enumerate(sine_list(tiles)):
                modes_ref[j, f, z] = tile
    tiles = []
    for z in range(count):
        first = (z % depth) * pieces
        tiles.append(
            jnp.concatenate(
                [
                    got_ref[i * space + z // depth, base : base + rows, :]
                    for i in range(first, first + pieces)
                ],
                axis=0,
            )
        )
    for z, tile in enumerate(sine_list(tiles)):
        start_ref[z] = tile
    for j in range(lo):
        state_ref[3, j] = jnp.broadcast_to(
            got_ref[j * space, base + rows : base + rows + 1, :], state_ref.shape[2:]
        )
    advance(dims, space, modes_ref, state_ref, x_ref, y_ref, lambda z: (start_ref[z],) * 3)


def advance(dims, space, modes_ref, state_ref, x_ref, y_ref, state_of):
    depth, groups, per, lo, pieces = dims
    count = depth * space
    plane = owner_weights(dims, space, x_ref, y_ref)
    steps = [state_ref[3, j] for j in range(lo)]
    weights = eigen(count)
    for z in range(count):
        neg = -(plane + float(weights[z]))
        guesses = [modes_ref[j, 0, z] for j in range(lo)]
        forced = [[modes_ref[j, 1 + m, z] for m in range(4)] for j in range(lo)]
        scaled = [steps[j] * neg for j in range(lo)]
        for i, tile in enumerate(march(guesses, forced, scaled, state_of(z), False)):
            state_ref[i, z] = tile


def middle_kernel(dims, space, modes_ref, start_ref, own_ref, came_ref, x_ref, y_ref, state_ref):
    lo = dims[3]
    head = lax.axis_index("hi") == 0
    for j in range(lo):
        state_ref[3, j] = own_ref[3, j]
    advance(
        dims,
        space,
        modes_ref,
        state_ref,
        x_ref,
        y_ref,
        lambda z: tuple(jnp.where(head, start_ref[z], came_ref[i, z]) for i in range(3)),
    )


def finish_kernel(dims, space, modes_ref, start_ref, own_ref, came_ref, x_ref, y_ref, out_ref, tmp_ref):
    depth, groups, per, lo, pieces = dims
    count = depth * space
    head = lax.axis_index("hi") == 0
    plane = owner_weights(dims, space, x_ref, y_ref)
    steps = [own_ref[3, j] for j in range(lo)]
    weights = eigen(count)
    for z in range(count):
        neg = -(plane + float(weights[z]))
        guesses = [modes_ref[j, 0, z] for j in range(lo)]
        forced = [[modes_ref[j, 1 + m, z] for m in range(4)] for j in range(lo)]
        scaled = [steps[j] * neg for j in range(lo)]
        start = start_ref[z]
        state = tuple(jnp.where(head, start, came_ref[i, z]) for i in range(3))
        for j, nodes in enumerate(march(guesses, forced, scaled, state, True)):
            for m in range(5):
                tmp_ref[j, m, z] = nodes[m]
    for j in range(lo):
        for m in range(5):
            tiles = sine_list([tmp_ref[j, m, z] for z in range(count)])
            for z in range(count):
                row = (m * depth + z % depth) * per
                out_ref[j * space + z // depth, row : row + per, :] = tiles[z]


def backward_kernel(dims, got_ref, right_ref, left_ref, out_ref):
    depth, groups, per, lo, pieces = dims
    rows, width = got_ref.shape[1:]
    mixed = times_sine(got_ref[...].reshape(groups * rows, width), right_ref[...])
    mixed = mixed.reshape(groups, rows, width)
    planes = [
        mixed[:, i * per : (i + 1) * per, :].reshape(groups * per, width)
        for i in range(5 * depth)
    ]
    for i in range(0, len(planes), 2):
        pair = sine_times(jnp.concatenate(planes[i : i + 2], axis=1), left_ref[...])
        out_ref[0, i // depth, i % depth] = pair[:, :width]
        out_ref[0, (i + 1) // depth, (i + 1) % depth] = pair[:, width:]


VMEM = pl.BlockSpec(memory_space=pltpu.VMEM)
SMEM = pl.BlockSpec(memory_space=pltpu.SMEM)


def call(kernel, shapes, count, scalars=0, scratch=()):
    many = isinstance(shapes, (list, tuple)) and isinstance(shapes[0], tuple)
    outs = [jax.ShapeDtypeStruct(s, jnp.float32) for s in (shapes if many else [shapes])]
    return pl.pallas_call(
        kernel,
        out_shape=outs if many else outs[0],
        in_specs=[SMEM] * scalars + [VMEM] * (count - scalars),
        out_specs=[VMEM] * len(outs) if many else VMEM,
        scratch_shapes=list(scratch),
    )


def body(initial, start_guess, forcing, step_size):
    depth, width_x, width_y = initial.shape
    space, lo, hi = (lax.axis_size(a) for a in ("space", "lo", "hi"))
    groups = space * lo
    per = width_x // groups
    pieces = lo // depth
    dims = (depth, groups, per, lo, pieces)
    count = depth * space
    right = jnp.asarray(right_table(width_y))
    left = jnp.asarray(left_table(width_x))
    x_weights = jnp.asarray(
        np.broadcast_to(eigen(width_x)[:, None], (width_x, width_y)).astype(np.float32)
    )
    y_weights = jnp.asarray(eigen(width_y)[None, :].astype(np.float32))

    rows = 5 * depth * per
    send = call(
        functools.partial(forward_kernel, dims), (groups, rows + TILE, width_y), 6, 1
    )(step_size, initial, start_guess, forcing, right, left)
    got = lax.all_to_all(send, ("lo", "space"), 0, 0, tiled=True)
    modes, start, state = call(
        functools.partial(gather_kernel, dims, space),
        [
            (lo, 5, count, per, width_y),
            (count, per, width_y),
            (4, max(count, lo), per, width_y),
        ],
        3,
    )(got, x_weights, y_weights)
    onward = [(i, i + 1) for i in range(hi - 1)]
    came = lax.ppermute(state[:3], "hi", onward)
    for _ in range(hi - 2):
        state = call(
            functools.partial(middle_kernel, dims, space), (4, max(count, lo), per, width_y), 6
        )(modes, start, state, came, x_weights, y_weights)
        came = lax.ppermute(state[:3], "hi", onward)
    send = call(
        functools.partial(finish_kernel, dims, space),
        (groups, rows, width_y),
        6,
        scratch=[pltpu.VMEM((lo, 5, count, per, width_y), jnp.float32)],
    )(modes, start, state, came, x_weights, y_weights)
    got = lax.all_to_all(send, ("lo", "space"), 0, 0, tiled=True)
    return call(
        functools.partial(backward_kernel, dims), (1, 5, depth, width_x, width_y), 3
    )(got, right, left)


def solution(mesh):
    steps, space = mesh.devices.shape
    time = ("hi", "lo")
    specs = (
        P("space", None, None),
        P(time, "space", None, None),
        P(time, None, "space", None, None),
        P(time),
    )

    def run(initial, start_guess, forcing, step_size):
        width = initial.shape[1]
        lo = max(
            d for d in range(1, steps + 1) if steps % d == 0 and width % (TILE * d * space) == 0
        )
        whole = Mesh(mesh.devices.reshape(steps // lo, lo, space), ("hi", "lo", "space"))
        return jax.shard_map(
            body,
            mesh=whole,
            in_specs=specs,
            out_specs=P(time, None, "space", None, None),
            check_vma=False,
        )(initial, start_guess, forcing, step_size)

    return run
```

```python
import functools
import math

import jax
import jax.numpy as jnp
import numpy as np
from jax import lax
from jax.experimental import pallas as pl
from jax.experimental.pallas import tpu as pltpu
from jax.sharding import Mesh
from jax.sharding import PartitionSpec as P

TILE = 8


def node_tables():
    radical = math.sqrt(3.0 / 7.0)
    node_times = [0.0, (1.0 - radical) / 2.0, 0.5, (1.0 + radical) / 2.0, 1.0]
    integrals = np.zeros((4, 5))
    for column in range(5):
        coeffs = [1.0]
        for other_index in range(5):
            if other_index == column:
                continue
            other_time = node_times[other_index]
            scaling = node_times[column] - other_time
            grown = [0.0] * (len(coeffs) + 1)
            for exponent in range(len(coeffs)):
                grown[exponent + 1] += coeffs[exponent] / scaling
                grown[exponent] -= coeffs[exponent] * other_time / scaling
            coeffs = grown
        for section in range(4):
            integrals[section, column] = sum(
                coeffs[exponent]
                * (node_times[section + 1] ** (exponent + 1) - node_times[section] ** (exponent + 1))
                / (exponent + 1)
                for exponent in range(len(coeffs))
            )
    coarse = [0.0, 0.5, 1.0]
    interp = np.zeros((5, 3))
    for column in range(3):
        for section in range(5):
            weight = 1.0
            for other_index in range(3):
                if other_index != column:
                    weight = (
                        weight
                        * (node_times[section] - coarse[other_index])
                        / (coarse[column] - coarse[other_index])
                    )
            interp[section, column] = weight
    return (np.array(node_times), integrals, interp)


TIMES, QUAD, INTERP = node_tables()
SPACING = np.diff(TIMES)
LEFT = QUAD[0] + QUAD[1]
RIGHT = QUAD[2] + QUAD[3]


def sine(length):
    index = np.arange(1, length + 1)
    return math.sqrt(2.0 / (length + 1)) * np.sin(math.pi / (length + 1) * np.outer(index, index))


def eigen(length):
    return 2.0 - 2.0 * np.cos(math.pi / (length + 1) * np.arange(1, length + 1))


def halves(matrix):
    high = matrix.astype(jnp.bfloat16).astype(np.float64)
    return high, matrix - high


def right_table(length):
    high, low = halves(sine(length))
    return np.block([[high, low], [high, np.zeros_like(high)]]).astype(jnp.bfloat16)


def left_table(length):
    high, low = halves(sine(length))
    return np.block([[high, high], [low, np.zeros_like(high)]]).astype(jnp.bfloat16)


def split(value):
    high = value.astype(jnp.bfloat16)
    return high, (value - high.astype(jnp.float32)).astype(jnp.bfloat16)


def times_sine(value, table):
    width = value.shape[-1]
    both = jnp.dot(
        jnp.concatenate(split(value), axis=1), table, preferred_element_type=jnp.float32
    )
    return both[:, :width] + both[:, width:]


def sine_times(value, table):
    width = value.shape[0]
    both = jnp.dot(
        table, jnp.concatenate(split(value), axis=0), preferred_element_type=jnp.float32
    )
    return both[:width] + both[width:]


def sine_list(values):
    count = len(values)
    matrix = sine(count)
    half = count // 2
    even = [values[i] + values[count - 1 - i] for i in range(half)]
    odd = [values[i] - values[count - 1 - i] for i in range(half)]
    middle = [values[half]] if count % 2 else []
    result = []
    for k in range(count):
        terms = even + middle if k % 2 == 0 else odd
        result.append(sum(float(matrix[k, i]) * term for i, term in enumerate(terms)))
    return result


def combine(weights, values):
    return sum(float(w) * v for w, v in zip(weights, values) if w != 0.0)


def sweep(first, nodes, forced, scaled):
    swept = [first]
    for m in range(4):
        inner = combine(QUAD[m], nodes)
        if m:
            inner = inner + float(SPACING[m]) * (swept[m] - nodes[m])
        swept.append(swept[m] + (scaled * inner + forced[m]))
    left = scaled * (combine(LEFT, swept) - 0.5 * swept[0]) + (forced[0] + forced[1])
    right = scaled * (combine(RIGHT, swept) - 0.5 * swept[2]) + (forced[2] + forced[3])
    return swept, left, right


def chain(start, left, right, gain):
    middle = gain * start + left
    return middle, gain * middle + right


def correct(swept, start, middle, ending):
    deltas = [start - swept[0], middle - swept[2], ending - swept[4]]
    return [
        start,
        swept[1] + combine(INTERP[1], deltas),
        middle,
        swept[3] + combine(INTERP[3], deltas),
        ending,
    ]


def march(guesses, forced, scaled, state, final):
    before, first, second = state
    fields = []
    for j, guess in enumerate(guesses):
        gain = 1.0 + 0.5 * scaled[j]
        swept, left, right = sweep(before, [before] + [guess] * 4, forced[j], scaled[j])
        middle, ending = chain(first, left, right, gain)
        nodes = correct(swept, first, middle, ending)
        swept, left, right = sweep(first, nodes, forced[j], scaled[j])
        middle, last = chain(second, left, right, gain)
        if final:
            fields.append(correct(swept, second, middle, last))
        before, first, second = guess, ending, last
    return fields if final else (before, first, second)


def forward_kernel(
    dims, step_ref, init_hbm, guess_hbm, forcing_hbm, right_hbm, left_hbm, out_ref,
    init_ref, guess_ref, forcing_ref, right_ref, left_ref, sems, table_sems,
):
    depth, groups, per, lo, pieces = dims
    tables = [
        pltpu.make_async_copy(right_hbm, right_ref, table_sems.at[0]),
        pltpu.make_async_copy(left_hbm, left_ref, table_sems.at[1]),
    ]
    copies = []
    for d in range(depth):
        copies.append(
            [
                pltpu.make_async_copy(init_hbm.at[d], init_ref.at[d], sems.at[d, 0]),
                pltpu.make_async_copy(guess_hbm.at[0, d], guess_ref.at[d], sems.at[d, 1]),
                pltpu.make_async_copy(forcing_hbm.at[0, :, d], forcing_ref.at[d], sems.at[d, 2]),
            ]
        )
        for copy in copies[d] + (tables if d == 0 else []):
            copy.start()
    step = step_ref[0]
    width = init_ref.shape[1]
    starts = []
    for d in range(depth):
        for copy in copies[d]:
            copy.wait()
        samples = [forcing_ref[d, j] for j in range(5)]
        planes = [init_ref[d], guess_ref[d]]
        planes += [step * combine(QUAD[m], samples) for m in range(4)]
        if d == 0:
            tables[0].wait()
        mixed = times_sine(jnp.concatenate(planes, axis=0), right_ref[...])
        for i in range(0, len(planes), 2):
            pair = jnp.concatenate(
                [mixed[k * width : (k + 1) * width] for k in (i, i + 1)], axis=1
            )
            if d == 0 and i == 0:
                tables[1].wait()
            pair = sine_times(pair, left_ref[...])
            half = pair.shape[1] // 2
            for f, plane in ((i - 1, pair[:, :half]), (i, pair[:, half:])):
                tiles = plane.reshape(groups, per, half)
                if f < 0:
                    starts.append(tiles)
                else:
                    row = (f * depth + d) * per
                    out_ref[:, row : row + per, :] = tiles
    mine = lax.axis_index("lo")
    rows = per // pieces
    share = None
    for i in range(lo):
        offset = (i % pieces) * rows
        tile = starts[i // pieces][:, offset : offset + rows]
        share = tile if share is None else jnp.where(mine == i, tile, share)
    base = 5 * depth * per
    out_ref[:, base : base + rows, :] = share
    out_ref[:, base + rows :, :] = jnp.full(
        (groups, out_ref.shape[1] - base - rows, out_ref.shape[2]), step, jnp.float32
    )


def to_modes(dims, space, got_ref, modes_ref, steps_ref):
    depth, groups, per, lo, pieces = dims
    base = 5 * depth * per + per // pieces
    for j in range(lo):
        for f in range(5):
            tiles = []
            for z in range(depth * space):
                row = (f * depth + z % depth) * per
                tiles.append(got_ref[j * space + z // depth, row : row + per, :])
            for z, tile in enumerate(sine_list(tiles)):
                modes_ref[j, f, z] = tile
        steps_ref[j] = jnp.broadcast_to(
            got_ref[j * space, base : base + 1, :], steps_ref.shape[1:]
        )


def initial_modes(dims, space, got_ref):
    depth, groups, per, lo, pieces = dims
    base = 5 * depth * per
    rows = per // pieces
    tiles = []
    for z in range(depth * space):
        first = (z % depth) * pieces
        parts = [
            got_ref[i * space + z // depth, base : base + rows, :]
            for i in range(first, first + pieces)
        ]
        tiles.append(jnp.concatenate(parts, axis=0))
    return sine_list(tiles)


def per_mode(dims, space, modes_ref, steps_ref, x_ref, y_ref, state_of, final):
    depth, groups, per, lo, pieces = dims
    owner = lax.axis_index("lo") * space + lax.axis_index("space")
    plane = x_ref[pl.ds(owner * per, per), :] + y_ref[...]
    steps = [steps_ref[j] for j in range(lo)]
    for z, weight in enumerate(eigen(depth * space)):
        neg = -(plane + float(weight))
        guesses = [modes_ref[j, 0, z] for j in range(lo)]
        forced = [[modes_ref[j, 1 + m, z] for m in range(4)] for j in range(lo)]
        yield z, march(guesses, forced, [s * neg for s in steps], state_of(z), final)


def first_kernel(dims, space, got_ref, x_ref, y_ref, state_ref, modes_ref, steps_ref, start_ref):
    @pl.when(lax.axis_index("hi") == 0)
    def _():
        to_modes(dims, space, got_ref, modes_ref, steps_ref)
        for z, tile in enumerate(initial_modes(dims, space, got_ref)):
            start_ref[z] = tile
        ends = per_mode(
            dims, space, modes_ref, steps_ref, x_ref, y_ref, lambda z: (start_ref[z],) * 3, False
        )
        for z, state in ends:
            for i in range(3):
                state_ref[i, z] = state[i]


def write_fields(dims, space, results, tmp_ref, out_ref):
    depth, groups, per, lo, pieces = dims
    for z, slices in results:
        for j, nodes in enumerate(slices):
            for m in range(5):
                tmp_ref[j, m, z] = nodes[m]
    for j in range(lo):
        for m in range(5):
            tiles = sine_list([tmp_ref[j, m, z] for z in range(depth * space)])
            for z, tile in enumerate(tiles):
                row = (m * depth + z % depth) * per
                out_ref[j * space + z // depth, row : row + per, :] = tile


def window_kernel(
    dims, space, got_ref, modes_in, steps_in, start_ref, x_ref, y_ref,
    modes_ref, steps_ref, out_ref, tmp_ref,
):
    head = lax.axis_index("hi") == 0

    @pl.when(head)
    def _():
        results = per_mode(
            dims, space, modes_ref, steps_ref, x_ref, y_ref, lambda z: (start_ref[z],) * 3, True
        )
        write_fields(dims, space, results, tmp_ref, out_ref)

    @pl.when(jnp.logical_not(head))
    def _():
        to_modes(dims, space, got_ref, modes_ref, steps_ref)


def middle_kernel(dims, space, state_in, modes_ref, steps_ref, came_ref, x_ref, y_ref, state_ref):
    @pl.when(lax.axis_index("hi") > 0)
    def _():
        ends = per_mode(
            dims, space, modes_ref, steps_ref, x_ref, y_ref,
            lambda z: tuple(came_ref[i, z] for i in range(3)), False,
        )
        for z, state in ends:
            for i in range(3):
                state_ref[i, z] = state[i]


def finish_kernel(
    dims, space, out_in, modes_ref, steps_ref, came_ref, x_ref, y_ref, out_ref, tmp_ref
):
    @pl.when(lax.axis_index("hi") > 0)
    def _():
        results = per_mode(
            dims, space, modes_ref, steps_ref, x_ref, y_ref,
            lambda z: tuple(came_ref[i, z] for i in range(3)), True,
        )
        write_fields(dims, space, results, tmp_ref, out_ref)


def backward_kernel(dims, got_ref, right_ref, left_ref, out_hbm, out_ref, sems):
    depth, groups, per, lo, pieces = dims
    rows, width = got_ref.shape[1:]
    copies = []
    for i in range(0, 5 * depth, 2):
        mixed = times_sine(
            got_ref[:, i * per : (i + 2) * per, :].reshape(groups * 2 * per, width), right_ref[...]
        ).reshape(groups, 2 * per, width)
        pair = jnp.concatenate(
            [
                mixed[:, :per].reshape(groups * per, width),
                mixed[:, per:].reshape(groups * per, width),
            ],
            axis=1,
        )
        pair = sine_times(pair, left_ref[...])
        for k, plane in ((i, pair[:, :width]), (i + 1, pair[:, width:])):
            out_ref[k] = plane
            copy = pltpu.make_async_copy(
                out_ref.at[k], out_hbm.at[0, k // depth, k % depth], sems.at[k]
            )
            copy.start()
            copies.append(copy)
    for copy in copies:
        copy.wait()


VMEM = pl.BlockSpec(memory_space=pltpu.VMEM)
SMEM = pl.BlockSpec(memory_space=pltpu.SMEM)
HBM = pl.BlockSpec(memory_space=pltpu.HBM)


def call(kernel, shapes, in_specs, scratch=(), out_spec=VMEM, aliases=None):
    return pl.pallas_call(
        kernel,
        out_shape=[jax.ShapeDtypeStruct(s, jnp.float32) for s in shapes],
        in_specs=in_specs,
        out_specs=[out_spec] * len(shapes),
        scratch_shapes=list(scratch),
        input_output_aliases=aliases or {},
        compiler_params=pltpu.CompilerParams(vmem_limit_bytes=12 * 2**20),
    )


def body(initial, start_guess, forcing, step_size):
    depth, width_x, width_y = initial.shape
    space, lo, hi = (lax.axis_size(a) for a in ("space", "lo", "hi"))
    groups = space * lo
    per = width_x // groups
    pieces = lo // depth
    dims = (depth, groups, per, lo, pieces)
    count = depth * space
    right = jnp.asarray(right_table(width_y))
    left = jnp.asarray(left_table(width_x))
    x_weights = jnp.asarray(
        np.broadcast_to(eigen(width_x)[:, None], (width_x, width_y)).astype(np.float32)
    )
    y_weights = jnp.asarray(eigen(width_y)[None, :].astype(np.float32))
    tile = (per, width_y)
    bind = functools.partial
    plane = (width_x, width_y)

    rows = 5 * depth * per
    (send,) = call(
        bind(forward_kernel, dims),
        [(groups, rows + TILE, width_y)],
        [SMEM] + [HBM] * 5,
        [
            pltpu.VMEM((depth, *plane), jnp.float32),
            pltpu.VMEM((depth, *plane), jnp.float32),
            pltpu.VMEM((depth, 5, *plane), jnp.float32),
            pltpu.VMEM(right.shape, right.dtype),
            pltpu.VMEM(left.shape, left.dtype),
            pltpu.SemaphoreType.DMA((depth, 3)),
            pltpu.SemaphoreType.DMA((2,)),
        ],
    )(step_size, initial, start_guess, forcing, right, left)
    got = lax.all_to_all(send, ("lo", "space"), 0, 0, tiled=True)
    state_shape, modes_shape, steps_shape = (3, count, *tile), (lo, 5, count, *tile), (lo, *tile)
    state, modes, steps, start = call(
        bind(first_kernel, dims, space),
        [state_shape, modes_shape, steps_shape, (count, *tile)],
        [VMEM] * 3,
    )(got, x_weights, y_weights)
    onward = [(i, i + 1) for i in range(hi - 1)]
    came = lax.ppermute(state, "hi", onward)
    field_scratch = [pltpu.VMEM((lo, 5, count, *tile), jnp.float32)]
    modes, steps, send = call(
        bind(window_kernel, dims, space),
        [modes_shape, steps_shape, (groups, rows, width_y)],
        [VMEM] * 6,
        field_scratch,
        aliases={1: 0, 2: 1},
    )(got, modes, steps, start, x_weights, y_weights)
    for _ in range(hi - 2):
        (state,) = call(
            bind(middle_kernel, dims, space), [state_shape], [VMEM] * 6, aliases={0: 0}
        )(state, modes, steps, came, x_weights, y_weights)
        came = lax.ppermute(state, "hi", onward)
    (send,) = call(
        bind(finish_kernel, dims, space),
        [(groups, rows, width_y)],
        [VMEM] * 6,
        field_scratch,
        aliases={0: 0},
    )(send, modes, steps, came, x_weights, y_weights)
    got = lax.all_to_all(send, ("lo", "space"), 0, 0, tiled=True)
    (fields,) = call(
        bind(backward_kernel, dims),
        [(1, 5, depth, width_x, width_y)],
        [VMEM] * 3,
        [
            pltpu.VMEM((5 * depth, *plane), jnp.float32),
            pltpu.SemaphoreType.DMA((5 * depth,)),
        ],
        HBM,
    )(got, right, left)
    return fields


def solution(mesh):
    steps, space = mesh.devices.shape
    time = ("hi", "lo")
    specs = (
        P("space", None, None),
        P(time, "space", None, None),
        P(time, None, "space", None, None),
        P(time),
    )

    def run(initial, start_guess, forcing, step_size):
        width = initial.shape[1]
        lo = max(
            d for d in range(1, steps + 1) if steps % d == 0 and width % (TILE * d * space) == 0
        )
        whole = Mesh(mesh.devices.reshape(steps // lo, lo, space), ("hi", "lo", "space"))
        return jax.shard_map(
            body,
            mesh=whole,
            in_specs=specs,
            out_specs=P(time, None, "space", None, None),
            check_vma=False,
        )(initial, start_guess, forcing, step_size)

    return run
```

```python
import functools
import math

import jax
import jax.numpy as jnp
import numpy as np
from jax import lax
from jax.experimental import pallas as pl
from jax.experimental.pallas import tpu as pltpu
from jax.sharding import Mesh
from jax.sharding import PartitionSpec as P

TILE = 8


def node_tables():
    radical = math.sqrt(3.0 / 7.0)
    node_times = [0.0, (1.0 - radical) / 2.0, 0.5, (1.0 + radical) / 2.0, 1.0]
    integrals = np.zeros((4, 5))
    for column in range(5):
        coeffs = [1.0]
        for other_index in range(5):
            if other_index == column:
                continue
            other_time = node_times[other_index]
            scaling = node_times[column] - other_time
            grown = [0.0] * (len(coeffs) + 1)
            for exponent in range(len(coeffs)):
                grown[exponent + 1] += coeffs[exponent] / scaling
                grown[exponent] -= coeffs[exponent] * other_time / scaling
            coeffs = grown
        for section in range(4):
            integrals[section, column] = sum(
                coeffs[exponent]
                * (node_times[section + 1] ** (exponent + 1) - node_times[section] ** (exponent + 1))
                / (exponent + 1)
                for exponent in range(len(coeffs))
            )
    coarse = [0.0, 0.5, 1.0]
    interp = np.zeros((5, 3))
    for column in range(3):
        for section in range(5):
            weight = 1.0
            for other_index in range(3):
                if other_index != column:
                    weight = (
                        weight
                        * (node_times[section] - coarse[other_index])
                        / (coarse[column] - coarse[other_index])
                    )
            interp[section, column] = weight
    return (np.array(node_times), integrals, interp)


TIMES, QUAD, INTERP = node_tables()
SPACING = np.diff(TIMES)
LEFT = QUAD[0] + QUAD[1]
RIGHT = QUAD[2] + QUAD[3]


def sine(length):
    index = np.arange(1, length + 1)
    return math.sqrt(2.0 / (length + 1)) * np.sin(math.pi / (length + 1) * np.outer(index, index))


def eigen(length):
    return 2.0 - 2.0 * np.cos(math.pi / (length + 1) * np.arange(1, length + 1))


def halves(matrix):
    high = matrix.astype(jnp.bfloat16).astype(np.float64)
    return high, matrix - high


def right_table(length):
    high, low = halves(sine(length))
    return np.block([[high, low], [high, np.zeros_like(high)]]).astype(jnp.bfloat16)


def left_table(length):
    high, low = halves(sine(length))
    return np.block([[high, high], [low, np.zeros_like(high)]]).astype(jnp.bfloat16)


def split(value):
    high = value.astype(jnp.bfloat16)
    return high, (value - high.astype(jnp.float32)).astype(jnp.bfloat16)


def times_sine(value, table):
    width = value.shape[-1]
    both = jnp.dot(
        jnp.concatenate(split(value), axis=1), table, preferred_element_type=jnp.float32
    )
    return both[:, :width] + both[:, width:]


def sine_times(value, table):
    width = value.shape[0]
    both = jnp.dot(
        table, jnp.concatenate(split(value), axis=0), preferred_element_type=jnp.float32
    )
    return both[:width] + both[width:]


def sine_list(values):
    count = len(values)
    matrix = sine(count)
    half = count // 2
    even = [values[i] + values[count - 1 - i] for i in range(half)]
    odd = [values[i] - values[count - 1 - i] for i in range(half)]
    middle = [values[half]] if count % 2 else []
    result = []
    for k in range(count):
        terms = even + middle if k % 2 == 0 else odd
        result.append(sum(float(matrix[k, i]) * term for i, term in enumerate(terms)))
    return result


def combine(weights, values):
    return sum(float(w) * v for w, v in zip(weights, values) if w != 0.0)


def sweep(first, nodes, forced, scaled):
    swept = [first]
    for m in range(4):
        inner = combine(QUAD[m], nodes)
        if m:
            inner = inner + float(SPACING[m]) * (swept[m] - nodes[m])
        swept.append(swept[m] + (scaled * inner + forced[m]))
    left = scaled * (combine(LEFT, swept) - 0.5 * swept[0]) + (forced[0] + forced[1])
    right = scaled * (combine(RIGHT, swept) - 0.5 * swept[2]) + (forced[2] + forced[3])
    return swept, left, right


def chain(start, left, right, gain):
    middle = gain * start + left
    return middle, gain * middle + right


def correct(swept, start, middle, ending):
    deltas = [start - swept[0], middle - swept[2], ending - swept[4]]
    return [
        start,
        swept[1] + combine(INTERP[1], deltas),
        middle,
        swept[3] + combine(INTERP[3], deltas),
        ending,
    ]


def march(guesses, forced, scaled, state, final):
    before, first, second = state
    fields = []
    for j, guess in enumerate(guesses):
        gain = 1.0 + 0.5 * scaled[j]
        swept, left, right = sweep(before, [before] + [guess] * 4, forced[j], scaled[j])
        middle, ending = chain(first, left, right, gain)
        nodes = correct(swept, first, middle, ending)
        swept, left, right = sweep(first, nodes, forced[j], scaled[j])
        middle, last = chain(second, left, right, gain)
        if final:
            fields.append(correct(swept, second, middle, last))
        before, first, second = guess, ending, last
    return fields if final else (before, first, second)


def forward_kernel(
    dims, step_ref, init_hbm, guess_hbm, forcing_hbm, right_hbm, left_hbm, out_ref,
    init_ref, guess_ref, forcing_ref, right_ref, left_ref, sems, table_sems,
):
    depth, groups, per, lo, pieces = dims
    tables = [
        pltpu.make_async_copy(right_hbm, right_ref, table_sems.at[0]),
        pltpu.make_async_copy(left_hbm, left_ref, table_sems.at[1]),
    ]
    copies = []
    for d in range(depth):
        copies.append(
            [
                pltpu.make_async_copy(init_hbm.at[d], init_ref.at[d], sems.at[d, 0]),
                pltpu.make_async_copy(guess_hbm.at[0, d], guess_ref.at[d], sems.at[d, 1]),
                pltpu.make_async_copy(forcing_hbm.at[0, :, d], forcing_ref.at[d], sems.at[d, 2]),
            ]
        )
        for copy in copies[d] + (tables if d == 0 else []):
            copy.start()
    step = step_ref[0]
    width = init_ref.shape[1]
    starts = []
    for d in range(depth):
        for copy in copies[d]:
            copy.wait()
        samples = [forcing_ref[d, j] for j in range(5)]
        planes = [init_ref[d], guess_ref[d]]
        planes += [step * combine(QUAD[m], samples) for m in range(4)]
        if d == 0:
            tables[0].wait()
        mixed = times_sine(jnp.concatenate(planes, axis=0), right_ref[...])
        for i in range(0, len(planes), 2):
            pair = jnp.concatenate(
                [mixed[k * width : (k + 1) * width] for k in (i, i + 1)], axis=1
            )
            if d == 0 and i == 0:
                tables[1].wait()
            pair = sine_times(pair, left_ref[...])
            half = pair.shape[1] // 2
            for f, plane in ((i - 1, pair[:, :half]), (i, pair[:, half:])):
                tiles = plane.reshape(groups, per, half)
                if f < 0:
                    starts.append(tiles)
                else:
                    row = (f * depth + d) * per
                    out_ref[:, row : row + per, :] = tiles
    mine = lax.axis_index("lo")
    rows = per // pieces
    share = None
    for i in range(lo):
        offset = (i % pieces) * rows
        tile = starts[i // pieces][:, offset : offset + rows]
        share = tile if share is None else jnp.where(mine == i, tile, share)
    base = 5 * depth * per
    out_ref[:, base : base + rows, :] = share
    out_ref[:, base + rows :, :] = jnp.full(
        (groups, out_ref.shape[1] - base - rows, out_ref.shape[2]), step, jnp.float32
    )


def to_modes(dims, space, got_ref, modes_ref, steps_ref):
    depth, groups, per, lo, pieces = dims
    base = 5 * depth * per + per // pieces
    for j in range(lo):
        for f in range(5):
            tiles = []
            for z in range(depth * space):
                row = (f * depth + z % depth) * per
                tiles.append(got_ref[j * space + z // depth, row : row + per, :])
            for z, tile in enumerate(sine_list(tiles)):
                modes_ref[j, f, z] = tile
        steps_ref[j] = jnp.broadcast_to(
            got_ref[j * space, base : base + 1, :], steps_ref.shape[1:]
        )


def initial_modes(dims, space, got_ref):
    depth, groups, per, lo, pieces = dims
    base = 5 * depth * per
    rows = per // pieces
    tiles = []
    for z in range(depth * space):
        first = (z % depth) * pieces
        parts = [
            got_ref[i * space + z // depth, base : base + rows, :]
            for i in range(first, first + pieces)
        ]
        tiles.append(jnp.concatenate(parts, axis=0))
    return sine_list(tiles)


def per_mode(dims, space, modes_ref, steps_ref, x_ref, y_ref, state_of, final):
    depth, groups, per, lo, pieces = dims
    owner = lax.axis_index("lo") * space + lax.axis_index("space")
    plane = x_ref[pl.ds(owner * per, per), :] + y_ref[...]
    steps = [steps_ref[j] for j in range(lo)]
    for z, weight in enumerate(eigen(depth * space)):
        neg = -(plane + float(weight))
        guesses = [modes_ref[j, 0, z] for j in range(lo)]
        forced = [[modes_ref[j, 1 + m, z] for m in range(4)] for j in range(lo)]
        yield z, march(guesses, forced, [s * neg for s in steps], state_of(z), final)


def first_kernel(dims, space, got_ref, x_ref, y_ref, state_ref, modes_ref, steps_ref, start_ref):
    @pl.when(lax.axis_index("hi") == 0)
    def _():
        to_modes(dims, space, got_ref, modes_ref, steps_ref)
        for z, tile in enumerate(initial_modes(dims, space, got_ref)):
            start_ref[z] = tile
        ends = per_mode(
            dims, space, modes_ref, steps_ref, x_ref, y_ref, lambda z: (start_ref[z],) * 3, False
        )
        for z, state in ends:
            for i in range(3):
                state_ref[i, z] = state[i]


def write_fields(dims, space, results, tmp_ref, out_ref):
    depth, groups, per, lo, pieces = dims
    for z, slices in results:
        for j, nodes in enumerate(slices):
            for m in range(5):
                tmp_ref[j, m, z] = nodes[m]
    for j in range(lo):
        for m in range(5):
            tiles = sine_list([tmp_ref[j, m, z] for z in range(depth * space)])
            for z, tile in enumerate(tiles):
                row = (m * depth + z % depth) * per
                out_ref[j * space + z // depth, row : row + per, :] = tile


def window_kernel(
    dims, space, got_ref, modes_in, steps_in, start_ref, x_ref, y_ref,
    modes_ref, steps_ref, out_ref, tmp_ref,
):
    head = lax.axis_index("hi") == 0

    @pl.when(head)
    def _():
        results = per_mode(
            dims, space, modes_ref, steps_ref, x_ref, y_ref, lambda z: (start_ref[z],) * 3, True
        )
        write_fields(dims, space, results, tmp_ref, out_ref)

    @pl.when(jnp.logical_not(head))
    def _():
        to_modes(dims, space, got_ref, modes_ref, steps_ref)


def middle_kernel(dims, space, state_in, modes_ref, steps_ref, came_ref, x_ref, y_ref, state_ref):
    @pl.when(lax.axis_index("hi") > 0)
    def _():
        ends = per_mode(
            dims, space, modes_ref, steps_ref, x_ref, y_ref,
            lambda z: tuple(came_ref[i, z] for i in range(3)), False,
        )
        for z, state in ends:
            for i in range(3):
                state_ref[i, z] = state[i]


def finish_kernel(
    dims, space, out_in, modes_ref, steps_ref, came_ref, x_ref, y_ref, out_ref, tmp_ref
):
    @pl.when(lax.axis_index("hi") > 0)
    def _():
        results = per_mode(
            dims, space, modes_ref, steps_ref, x_ref, y_ref,
            lambda z: tuple(came_ref[i, z] for i in range(3)), True,
        )
        write_fields(dims, space, results, tmp_ref, out_ref)


def backward_kernel(dims, got_ref, right_ref, left_ref, out_hbm, out_ref, sems):
    depth, groups, per, lo, pieces = dims
    rows, width = got_ref.shape[1:]
    copies = []
    for i in range(0, 5 * depth, 2):
        mixed = times_sine(
            got_ref[:, i * per : (i + 2) * per, :].reshape(groups * 2 * per, width), right_ref[...]
        ).reshape(groups, 2 * per, width)
        pair = jnp.concatenate(
            [
                mixed[:, :per].reshape(groups * per, width),
                mixed[:, per:].reshape(groups * per, width),
            ],
            axis=1,
        )
        pair = sine_times(pair, left_ref[...])
        for k, plane in ((i, pair[:, :width]), (i + 1, pair[:, width:])):
            out_ref[k] = plane
            copy = pltpu.make_async_copy(
                out_ref.at[k], out_hbm.at[0, k // depth, k % depth], sems.at[k]
            )
            copy.start()
            copies.append(copy)
    for copy in copies:
        copy.wait()


VMEM = pl.BlockSpec(memory_space=pltpu.VMEM)
SMEM = pl.BlockSpec(memory_space=pltpu.SMEM)
HBM = pl.BlockSpec(memory_space=pltpu.HBM)


def in_hbm(value):
    return pltpu.with_memory_space_constraint(value, pltpu.HBM)


def call(kernel, shapes, in_specs, scratch=(), out_spec=VMEM, aliases=None):
    return pl.pallas_call(
        kernel,
        out_shape=[jax.ShapeDtypeStruct(s, jnp.float32) for s in shapes],
        in_specs=in_specs,
        out_specs=[out_spec] * len(shapes),
        scratch_shapes=list(scratch),
        input_output_aliases=aliases or {},
        compiler_params=pltpu.CompilerParams(vmem_limit_bytes=12 * 2**20),
    )


def body(initial, start_guess, forcing, step_size):
    depth, width_x, width_y = initial.shape
    space, lo, hi = (lax.axis_size(a) for a in ("space", "lo", "hi"))
    groups = space * lo
    per = width_x // groups
    pieces = lo // depth
    dims = (depth, groups, per, lo, pieces)
    count = depth * space
    right = jnp.asarray(right_table(width_y))
    left = jnp.asarray(left_table(width_x))
    x_weights = jnp.asarray(
        np.broadcast_to(eigen(width_x)[:, None], (width_x, width_y)).astype(np.float32)
    )
    y_weights = jnp.asarray(eigen(width_y)[None, :].astype(np.float32))
    tile = (per, width_y)
    bind = functools.partial
    plane = (width_x, width_y)

    rows = 5 * depth * per
    (send,) = call(
        bind(forward_kernel, dims),
        [(groups, rows + TILE, width_y)],
        [SMEM] + [HBM] * 5,
        [
            pltpu.VMEM((depth, *plane), jnp.float32),
            pltpu.VMEM((depth, *plane), jnp.float32),
            pltpu.VMEM((depth, 5, *plane), jnp.float32),
            pltpu.VMEM(right.shape, right.dtype),
            pltpu.VMEM(left.shape, left.dtype),
            pltpu.SemaphoreType.DMA((depth, 3)),
            pltpu.SemaphoreType.DMA((2,)),
        ],
    )(step_size, *(in_hbm(a) for a in (initial, start_guess, forcing, right, left)))
    got = lax.all_to_all(send, ("lo", "space"), 0, 0, tiled=True)
    state_shape, modes_shape, steps_shape = (3, count, *tile), (lo, 5, count, *tile), (lo, *tile)
    state, modes, steps, start = call(
        bind(first_kernel, dims, space),
        [state_shape, modes_shape, steps_shape, (count, *tile)],
        [VMEM] * 3,
    )(got, x_weights, y_weights)
    onward = [(i, i + 1) for i in range(hi - 1)]
    came = lax.ppermute(state, "hi", onward)
    field_scratch = [pltpu.VMEM((lo, 5, count, *tile), jnp.float32)]
    modes, steps, send = call(
        bind(window_kernel, dims, space),
        [modes_shape, steps_shape, (groups, rows, width_y)],
        [VMEM] * 6,
        field_scratch,
        aliases={1: 0, 2: 1},
    )(got, modes, steps, start, x_weights, y_weights)
    for _ in range(hi - 2):
        (state,) = call(
            bind(middle_kernel, dims, space), [state_shape], [VMEM] * 6, aliases={0: 0}
        )(state, modes, steps, came, x_weights, y_weights)
        came = lax.ppermute(state, "hi", onward)
    (send,) = call(
        bind(finish_kernel, dims, space),
        [(groups, rows, width_y)],
        [VMEM] * 6,
        field_scratch,
        aliases={0: 0},
    )(send, modes, steps, came, x_weights, y_weights)
    got = lax.all_to_all(send, ("lo", "space"), 0, 0, tiled=True)
    (fields,) = call(
        bind(backward_kernel, dims),
        [(1, 5, depth, width_x, width_y)],
        [VMEM] * 3,
        [
            pltpu.VMEM((5 * depth, *plane), jnp.float32),
            pltpu.SemaphoreType.DMA((5 * depth,)),
        ],
        HBM,
    )(got, right, left)
    return fields


def solution(mesh):
    steps, space = mesh.devices.shape
    time = ("hi", "lo")
    specs = (
        P("space", None, None),
        P(time, "space", None, None),
        P(time, None, "space", None, None),
        P(time),
    )

    def run(initial, start_guess, forcing, step_size):
        width = initial.shape[1]
        lo = max(
            d for d in range(1, steps + 1) if steps % d == 0 and width % (TILE * d * space) == 0
        )
        whole = Mesh(mesh.devices.reshape(steps // lo, lo, space), ("hi", "lo", "space"))
        return jax.shard_map(
            body,
            mesh=whole,
            in_specs=specs,
            out_specs=P(time, None, "space", None, None),
            check_vma=False,
        )(initial, start_guess, forcing, step_size)

    return run
```

```python
import functools
import math

import jax
import jax.numpy as jnp
import numpy as np
from jax import lax
from jax.experimental import pallas as pl
from jax.experimental.pallas import tpu as pltpu
from jax.sharding import Mesh
from jax.sharding import PartitionSpec as P

TILE = 8


def node_tables():
    radical = math.sqrt(3.0 / 7.0)
    node_times = [0.0, (1.0 - radical) / 2.0, 0.5, (1.0 + radical) / 2.0, 1.0]
    integrals = np.zeros((4, 5))
    for column in range(5):
        coeffs = [1.0]
        for other_index in range(5):
            if other_index == column:
                continue
            other_time = node_times[other_index]
            scaling = node_times[column] - other_time
            grown = [0.0] * (len(coeffs) + 1)
            for exponent in range(len(coeffs)):
                grown[exponent + 1] += coeffs[exponent] / scaling
                grown[exponent] -= coeffs[exponent] * other_time / scaling
            coeffs = grown
        for section in range(4):
            integrals[section, column] = sum(
                coeffs[exponent]
                * (node_times[section + 1] ** (exponent + 1) - node_times[section] ** (exponent + 1))
                / (exponent + 1)
                for exponent in range(len(coeffs))
            )
    coarse = [0.0, 0.5, 1.0]
    interp = np.zeros((5, 3))
    for column in range(3):
        for section in range(5):
            weight = 1.0
            for other_index in range(3):
                if other_index != column:
                    weight = (
                        weight
                        * (node_times[section] - coarse[other_index])
                        / (coarse[column] - coarse[other_index])
                    )
            interp[section, column] = weight
    return (np.array(node_times), integrals, interp)


TIMES, QUAD, INTERP = node_tables()
SPACING = np.diff(TIMES)
LEFT = QUAD[0] + QUAD[1]
RIGHT = QUAD[2] + QUAD[3]


def sine(length):
    index = np.arange(1, length + 1)
    return math.sqrt(2.0 / (length + 1)) * np.sin(math.pi / (length + 1) * np.outer(index, index))


def eigen(length):
    return 2.0 - 2.0 * np.cos(math.pi / (length + 1) * np.arange(1, length + 1))


def sine_parts(length):
    matrix = sine(length)
    high = matrix.astype(jnp.bfloat16)
    low = (matrix - high.astype(np.float64)).astype(jnp.bfloat16)
    return np.stack([high, low])


def right_table(length):
    high, low = sine_parts(length)
    return np.block([[high, low], [high, np.zeros_like(high)]])


def left_table(length):
    high, low = sine_parts(length)
    return np.block([[high, high], [low, np.zeros_like(high)]])


def split(value):
    high = value.astype(jnp.bfloat16)
    return high, (value - high.astype(jnp.float32)).astype(jnp.bfloat16)


def times_sine(value, table):
    width = value.shape[-1]
    both = jnp.dot(
        jnp.concatenate(split(value), axis=1), table, preferred_element_type=jnp.float32
    )
    return both[:, :width] + both[:, width:]


def sine_times(value, table):
    width = value.shape[0]
    both = jnp.dot(
        table, jnp.concatenate(split(value), axis=0), preferred_element_type=jnp.float32
    )
    return both[:width] + both[width:]


def sine_list(values):
    count = len(values)
    matrix = sine(count)
    half = count // 2
    even = [values[i] + values[count - 1 - i] for i in range(half)]
    odd = [values[i] - values[count - 1 - i] for i in range(half)]
    middle = [values[half]] if count % 2 else []
    result = []
    for k in range(count):
        terms = even + middle if k % 2 == 0 else odd
        result.append(sum(float(matrix[k, i]) * term for i, term in enumerate(terms)))
    return result


def zero(value):
    return isinstance(value, float) and value == 0.0


def plus(*values):
    values = [v for v in values if not zero(v)]
    return sum(values[1:], values[0]) if values else 0.0


def times(factor, value):
    return 0.0 if zero(factor) or zero(value) else factor * value


def minus(value, other):
    return value if zero(other) else plus(value, -other)


def combine(weights, values):
    return plus(*(times(float(w), v) for w, v in zip(weights, values)))


def sweep(first, nodes, forced, scaled):
    swept = [first]
    for m in range(4):
        inner = combine(QUAD[m], nodes)
        if m:
            inner = plus(inner, times(float(SPACING[m]), minus(swept[m], nodes[m])))
        swept.append(plus(swept[m], times(scaled, inner), forced[m]))
    left = plus(times(scaled, combine(LEFT - 0.5 * np.eye(5)[0], swept)), *forced[:2])
    right = plus(times(scaled, combine(RIGHT - 0.5 * np.eye(5)[2], swept)), *forced[2:])
    return swept, left, right


def chain(start, left, right, gain):
    middle = plus(times(gain, start), left)
    return middle, plus(times(gain, middle), right)


def correct(swept, start, middle, ending):
    deltas = [minus(start, swept[0]), minus(middle, swept[2]), minus(ending, swept[4])]
    return [
        start,
        plus(swept[1], combine(INTERP[1], deltas)),
        middle,
        plus(swept[3], combine(INTERP[3], deltas)),
        ending,
    ]


def march(guesses, forced, scaled, state, final):
    before, first, second = state
    fields = []
    for j, guess in enumerate(guesses):
        gain = 1.0 + 0.5 * scaled[j]
        swept, left, right = sweep(before, [before] + [guess] * 4, forced[j], scaled[j])
        middle, ending = chain(first, left, right, gain)
        nodes = correct(swept, first, middle, ending)
        swept, left, right = sweep(first, nodes, forced[j], scaled[j])
        middle, last = chain(second, left, right, gain)
        if final:
            fields.append(correct(swept, second, middle, last))
        before, first, second = guess, ending, last
    return fields if final else (before, first, second)


def responses(scaled):
    nothing = [0.0] * len(scaled)
    return [
        march(nothing, [[0.0] * 4] * len(scaled), scaled, [float(i == k) for k in range(3)], True)
        for i in range(3)
    ]


def distinct(lo):
    return [(j, m) for j in range(lo) for m in range(5) if j == 0 or m]


def forward_kernel(
    dims, step_ref, init_hbm, guess_hbm, forcing_hbm, parts_hbm, out_ref,
    init_ref, guess_ref, forcing_ref, parts_ref, table_ref, sems, plane_sems,
):
    depth, groups, per, lo, space = dims[:5]
    pieces = lo // depth
    copies = [
        pltpu.make_async_copy(parts_hbm, parts_ref, sems.at[0]),
        pltpu.make_async_copy(init_hbm, init_ref, sems.at[1]),
        pltpu.make_async_copy(guess_hbm.at[0], guess_ref, sems.at[2]),
    ]
    copies += [
        pltpu.make_async_copy(forcing_hbm.at[0, :, d], forcing_ref.at[d], plane_sems.at[d])
        for d in range(depth)
    ]
    for copy in copies:
        copy.start()
    step = step_ref[0]
    width = parts_ref.shape[1]

    copies[0].wait()
    high, low = parts_ref[0], parts_ref[1]
    table_ref[:width, :width] = high
    table_ref[:width, width:] = high
    table_ref[width:, :width] = low
    table_ref[width:, width:] = jnp.zeros_like(low)

    def transform(planes):
        joined = sine_times(jnp.concatenate(planes, axis=1), table_ref[...])
        half = joined.shape[1] // len(planes)
        return [
            joined[:, i * half : (i + 1) * half].reshape(groups, per, half)
            for i in range(len(planes))
        ]

    def put(field, d, tiles):
        row = (field * depth + d) * per
        out_ref[:, row : row + per, :] = tiles

    copies[1].wait()
    starts = transform([init_ref[d] for d in range(depth)])
    mine = lax.axis_index("lo")
    rows = per // pieces
    share = None
    for i in range(lo):
        offset = (i % pieces) * rows
        tile = starts[i // pieces][:, offset : offset + rows]
        share = tile if share is None else jnp.where(mine == i, tile, share)
    base = 5 * depth * per
    out_ref[:, base : base + rows, :] = share
    out_ref[:, base + rows :, :] = jnp.full(
        (groups, out_ref.shape[1] - base - rows, out_ref.shape[2]), step, jnp.float32
    )
    copies[2].wait()
    for d, tiles in enumerate(transform([guess_ref[d] for d in range(depth)])):
        put(0, d, tiles)
    for d in range(depth):
        copies[3 + d].wait()
        samples = [forcing_ref[d, j] for j in range(5)]
        for m in (0, 2):
            pair = [step * combine(QUAD[k], samples) for k in (m, m + 1)]
            for k, tiles in enumerate(transform(pair)):
                put(1 + m + k, d, tiles)


def source(dims, j, z):
    depth, groups, per, lo, space, cores = dims
    device = z // depth
    return (device % cores * lo + j) * (space // cores) + device // cores, z % depth


def to_modes(dims, got_ref, right_ref, modes_ref, steps_ref):
    depth, groups, per, lo, space, cores = dims
    base = 5 * depth * per + per // (lo // depth)
    count = depth * space
    for j in range(lo):
        columns = []
        for f in range(5):
            tiles = []
            for z in range(count):
                device, d = source(dims, j, z)
                row = (f * depth + d) * per
                tiles.append(got_ref[device, row : row + per, :])
            columns += sine_list(tiles)
        mixed = times_sine(jnp.concatenate(columns, axis=0), right_ref[...])
        modes_ref[j] = mixed.reshape(5, count, per, mixed.shape[1])
        steps_ref[j] = jnp.broadcast_to(
            got_ref[source(dims, j, 0)[0], base : base + 1, :], steps_ref.shape[1:]
        )


def initial_modes(dims, got_ref, right_ref):
    depth, groups, per, lo, space, cores = dims
    pieces = lo // depth
    base = 5 * depth * per
    rows = per // pieces
    tiles = []
    for z in range(depth * space):
        first = (z % depth) * pieces
        parts = [
            got_ref[source(dims, i, z)[0], base : base + rows, :]
            for i in range(first, first + pieces)
        ]
        tiles.append(jnp.concatenate(parts, axis=0))
    mixed = times_sine(jnp.concatenate(sine_list(tiles), axis=0), right_ref[...])
    return mixed.reshape(depth * space, per, mixed.shape[1])


def per_mode(dims, modes_ref, steps_ref, x_ref, y_ref):
    depth, groups, per, lo, space, cores = dims
    device = lax.axis_index("core") * lo + lax.axis_index("lo")
    owner = device * (space // cores) + lax.axis_index("chip")
    plane = x_ref[pl.ds(owner * per, per), :] + y_ref[...]
    steps = [steps_ref[j] for j in range(lo)]
    for z, weight in enumerate(eigen(depth * space)):
        neg = -(plane + float(weight))
        guesses = [modes_ref[j, 0, z] for j in range(lo)]
        forced = [[modes_ref[j, 1 + m, z] for m in range(4)] for j in range(lo)]
        yield z, guesses, forced, [s * neg for s in steps]


def put_fields(dims, fields_of, out_ref):
    depth, groups, per, lo, space, cores = dims
    for j, m in distinct(lo):
        for z, tile in enumerate(sine_list(fields_of(j, m))):
            places = [(j, m)] + ([(j + 1, 0)] if m == 4 and j + 1 < lo else [])
            for slot, node in places:
                device, d = source(dims, slot, z)
                row = (node * depth + d) * per
                out_ref[device, row : row + per, :] = tile


def first_kernel(
    dims, got_ref, right_ref, x_ref, y_ref, state_ref, modes_ref, steps_ref, start_ref
):
    @pl.when(lax.axis_index("hi") == 0)
    def _():
        to_modes(dims, got_ref, right_ref, modes_ref, steps_ref)
        start_ref[...] = initial_modes(dims, got_ref, right_ref)
        for z, guesses, forced, scaled in per_mode(dims, modes_ref, steps_ref, x_ref, y_ref):
            state = march(guesses, forced, scaled, (start_ref[z],) * 3, False)
            for i in range(3):
                state_ref[i, z] = state[i]


def window_kernel(
    dims, got_ref, modes_in, steps_in, start_ref, right_ref, x_ref, y_ref,
    modes_ref, steps_ref, out_ref, part_ref, unit_ref,
):
    depth, groups, per, lo, space, cores = dims
    head = lax.axis_index("hi") == 0

    @pl.when(head)
    def _():
        for z, guesses, forced, scaled in per_mode(dims, modes_ref, steps_ref, x_ref, y_ref):
            fields = march(guesses, forced, scaled, (start_ref[z],) * 3, True)
            for k, (j, m) in enumerate(distinct(lo)):
                part_ref[k, z] = fields[j][m]
        where = {place: k for k, place in enumerate(distinct(lo))}
        put_fields(
            dims,
            lambda j, m: [part_ref[where[j, m], z] for z in range(depth * space)],
            out_ref,
        )

    @pl.when(jnp.logical_not(head))
    def _():
        to_modes(dims, got_ref, right_ref, modes_ref, steps_ref)
        for z, guesses, forced, scaled in per_mode(dims, modes_ref, steps_ref, x_ref, y_ref):
            fields = march(guesses, forced, scaled, (0.0,) * 3, True)
            added = responses(scaled)
            for k, (j, m) in enumerate(distinct(lo)):
                if not zero(fields[j][m]):
                    part_ref[k, z] = fields[j][m]
                for i in range(3):
                    if not isinstance(added[i][j][m], float):
                        unit_ref[i, k, z] = added[i][j][m]


def middle_kernel(dims, state_in, modes_ref, steps_ref, came_ref, x_ref, y_ref, state_ref):
    @pl.when(lax.axis_index("hi") > 0)
    def _():
        for z, guesses, forced, scaled in per_mode(dims, modes_ref, steps_ref, x_ref, y_ref):
            came = tuple(came_ref[i, z] for i in range(3))
            state = march(guesses, forced, scaled, came, False)
            for i in range(3):
                state_ref[i, z] = state[i]


def finish_kernel(dims, out_in, part_ref, unit_ref, came_ref, out_ref):
    depth, groups, per, lo, space, cores = dims

    @pl.when(lax.axis_index("hi") > 0)
    def _():
        stand = [np.float32(0.5)] * lo
        fields = march(stand, [stand[:1] * 4] * lo, stand, (0.0,) * 3, True)
        added = responses(stand)
        where = {place: k for k, place in enumerate(distinct(lo))}

        def fields_of(j, m):
            k = where[j, m]
            tiles = []
            for z in range(depth * space):
                terms = [] if zero(fields[j][m]) else [part_ref[k, z]]
                for i in range(3):
                    unit = added[i][j][m]
                    if not isinstance(unit, float):
                        unit = unit_ref[i, k, z]
                    terms.append(times(unit, came_ref[i, z]))
                tiles.append(plus(*terms))
            return tiles

        put_fields(dims, fields_of, out_ref)


def backward_kernel(dims, got_ref, right_ref, left_ref, out_hbm, out_ref, sems):
    depth, groups, per = dims[:3]
    rows, width = got_ref.shape[1:]
    copies = []
    for i in range(0, 5 * depth, 2):
        mixed = times_sine(
            got_ref[:, i * per : (i + 2) * per, :].reshape(groups * 2 * per, width), right_ref[...]
        ).reshape(groups, 2 * per, width)
        pair = jnp.concatenate(
            [
                mixed[:, :per].reshape(groups * per, width),
                mixed[:, per:].reshape(groups * per, width),
            ],
            axis=1,
        )
        pair = sine_times(pair, left_ref[...])
        for k, plane in ((i, pair[:, :width]), (i + 1, pair[:, width:])):
            out_ref[k] = plane
            copy = pltpu.make_async_copy(
                out_ref.at[k], out_hbm.at[0, k // depth, k % depth], sems.at[k]
            )
            copy.start()
            copies.append(copy)
    for copy in copies:
        copy.wait()


VMEM = pl.BlockSpec(memory_space=pltpu.VMEM)
SMEM = pl.BlockSpec(memory_space=pltpu.SMEM)
HBM = pl.BlockSpec(memory_space=pltpu.HBM)


def in_hbm(value):
    return pltpu.with_memory_space_constraint(value, pltpu.HBM)


def call(kernel, shapes, in_specs, scratch=(), out_spec=VMEM, aliases=None):
    return pl.pallas_call(
        kernel,
        out_shape=[jax.ShapeDtypeStruct(s, jnp.float32) for s in shapes],
        in_specs=in_specs,
        out_specs=[out_spec] * len(shapes),
        scratch_shapes=list(scratch),
        input_output_aliases=aliases or {},
        compiler_params=pltpu.CompilerParams(vmem_limit_bytes=12 * 2**20),
    )


def body(initial, start_guess, forcing, step_size):
    depth, width_x, width_y = initial.shape
    hi, lo, chips, cores = (lax.axis_size(a) for a in ("hi", "lo", "chip", "core"))
    space = chips * cores
    groups = space * lo
    per = width_x // groups
    dims = (depth, groups, per, lo, space, cores)
    count = depth * space
    parts = jnp.asarray(sine_parts(width_x))
    right = jnp.asarray(right_table(width_y))
    left = jnp.asarray(left_table(width_x))
    x_weights = jnp.asarray(
        np.broadcast_to(eigen(width_x)[:, None], (width_x, width_y)).astype(np.float32)
    )
    y_weights = jnp.asarray(eigen(width_y)[None, :].astype(np.float32))
    tile = (per, width_y)
    plane = (width_x, width_y)
    bind = functools.partial

    rows = 5 * depth * per
    (send,) = call(
        bind(forward_kernel, dims),
        [(groups, rows + TILE, width_y)],
        [SMEM] + [HBM] * 4,
        [
            pltpu.VMEM((depth, *plane), jnp.float32),
            pltpu.VMEM((depth, *plane), jnp.float32),
            pltpu.VMEM((depth, 5, *plane), jnp.float32),
            pltpu.VMEM(parts.shape, parts.dtype),
            pltpu.VMEM(left.shape, left.dtype),
            pltpu.SemaphoreType.DMA((3,)),
            pltpu.SemaphoreType.DMA((depth,)),
        ],
    )(step_size, *(in_hbm(a) for a in (initial, start_guess, forcing, parts)))
    members = ("core", "lo", "chip")
    got = lax.all_to_all(send, members, 0, 0, tiled=True)
    state_shape, modes_shape, steps_shape = (3, count, *tile), (lo, 5, count, *tile), (lo, *tile)
    state, modes, steps, start = call(
        bind(first_kernel, dims),
        [state_shape, modes_shape, steps_shape, (count, *tile)],
        [VMEM] * 4,
    )(got, right, x_weights, y_weights)
    onward = [(i, i + 1) for i in range(hi - 1)]
    came = lax.ppermute(state, "hi", onward)
    kinds = len(distinct(lo))
    modes, steps, send, part, unit = call(
        bind(window_kernel, dims),
        [
            modes_shape,
            steps_shape,
            (groups, rows, width_y),
            (kinds, count, *tile),
            (3, kinds, count, *tile),
        ],
        [VMEM] * 7,
        aliases={1: 0, 2: 1},
    )(got, modes, steps, start, right, x_weights, y_weights)
    for _ in range(hi - 2):
        (state,) = call(bind(middle_kernel, dims), [state_shape], [VMEM] * 6, aliases={0: 0})(
            state, modes, steps, came, x_weights, y_weights
        )
        came = lax.ppermute(state, "hi", onward)
    (send,) = call(
        bind(finish_kernel, dims), [(groups, rows, width_y)], [VMEM] * 4, aliases={0: 0}
    )(send, part, unit, came)
    got = lax.all_to_all(send, members, 0, 0, tiled=True)
    (fields,) = call(
        bind(backward_kernel, dims),
        [(1, 5, depth, width_x, width_y)],
        [VMEM] * 3,
        [
            pltpu.VMEM((5 * depth, *plane), jnp.float32),
            pltpu.SemaphoreType.DMA((5 * depth,)),
        ],
        HBM,
    )(got, right, left)
    return fields


def solution(mesh):
    steps, space = mesh.devices.shape
    cores = 2 if space % 2 == 0 else 1
    time, slabs = ("hi", "lo"), ("chip", "core")
    specs = (P(slabs), P(time, slabs), P(time, None, slabs), P(time))

    def run(initial, start_guess, forcing, step_size):
        width = initial.shape[1]
        lo = max(
            d for d in range(1, steps + 1) if steps % d == 0 and width % (TILE * d * space) == 0
        )
        shape = (steps // lo, lo, space // cores, cores)
        whole = Mesh(mesh.devices.reshape(shape), time + slabs)
        return jax.shard_map(
            body, mesh=whole, in_specs=specs, out_specs=P(time, None, slabs), check_vma=False
        )(initial, start_guess, forcing, step_size)

    return run
```

```python
import functools
import math

import jax
import jax.numpy as jnp
import numpy as np
from jax import lax
from jax.experimental import pallas as pl
from jax.experimental.pallas import tpu as pltpu
from jax.sharding import Mesh
from jax.sharding import PartitionSpec as P

TILE = 8


def node_tables():
    radical = math.sqrt(3.0 / 7.0)
    node_times = [0.0, (1.0 - radical) / 2.0, 0.5, (1.0 + radical) / 2.0, 1.0]
    integrals = np.zeros((4, 5))
    for column in range(5):
        coeffs = [1.0]
        for other_index in range(5):
            if other_index == column:
                continue
            other_time = node_times[other_index]
            scaling = node_times[column] - other_time
            grown = [0.0] * (len(coeffs) + 1)
            for exponent in range(len(coeffs)):
                grown[exponent + 1] += coeffs[exponent] / scaling
                grown[exponent] -= coeffs[exponent] * other_time / scaling
            coeffs = grown
        for section in range(4):
            integrals[section, column] = sum(
                coeffs[exponent]
                * (node_times[section + 1] ** (exponent + 1) - node_times[section] ** (exponent + 1))
                / (exponent + 1)
                for exponent in range(len(coeffs))
            )
    coarse = [0.0, 0.5, 1.0]
    interp = np.zeros((5, 3))
    for column in range(3):
        for section in range(5):
            weight = 1.0
            for other_index in range(3):
                if other_index != column:
                    weight = (
                        weight
                        * (node_times[section] - coarse[other_index])
                        / (coarse[column] - coarse[other_index])
                    )
            interp[section, column] = weight
    return (np.array(node_times), integrals, interp)


TIMES, QUAD, INTERP = node_tables()
SPACING = np.diff(TIMES)
LEFT = QUAD[0] + QUAD[1]
RIGHT = QUAD[2] + QUAD[3]


def sine(length):
    index = np.arange(1, length + 1)
    return math.sqrt(2.0 / (length + 1)) * np.sin(math.pi / (length + 1) * np.outer(index, index))


def eigen(length):
    return 2.0 - 2.0 * np.cos(math.pi / (length + 1) * np.arange(1, length + 1))


def sine_parts(length):
    matrix = sine(length)
    high = matrix.astype(jnp.bfloat16)
    low = (matrix - high.astype(np.float64)).astype(jnp.bfloat16)
    return np.stack([high, low])


def right_table(length):
    high, low = sine_parts(length)
    return np.block([[high, low], [high, np.zeros_like(high)]])


def left_table(length):
    high, low = sine_parts(length)
    return np.block([[high, high], [low, np.zeros_like(high)]])


def split(value):
    high = value.astype(jnp.bfloat16)
    return high, (value - high.astype(jnp.float32)).astype(jnp.bfloat16)


def times_sine(value, table):
    width = value.shape[-1]
    both = jnp.dot(
        jnp.concatenate(split(value), axis=1), table, preferred_element_type=jnp.float32
    )
    return both[:, :width] + both[:, width:]


def sine_times(value, table):
    width = value.shape[0]
    both = jnp.dot(
        table, jnp.concatenate(split(value), axis=0), preferred_element_type=jnp.float32
    )
    return both[:width] + both[width:]


def sine_list(values):
    count = len(values)
    matrix = sine(count)
    half = count // 2
    even = [values[i] + values[count - 1 - i] for i in range(half)]
    odd = [values[i] - values[count - 1 - i] for i in range(half)]
    middle = [values[half]] if count % 2 else []
    result = []
    for k in range(count):
        terms = even + middle if k % 2 == 0 else odd
        result.append(sum(float(matrix[k, i]) * term for i, term in enumerate(terms)))
    return result


def zero(value):
    return isinstance(value, float) and value == 0.0


def plus(*values):
    values = [v for v in values if not zero(v)]
    return sum(values[1:], values[0]) if values else 0.0


def times(factor, value):
    return 0.0 if zero(factor) or zero(value) else factor * value


def minus(value, other):
    return value if zero(other) else plus(value, -other)


def combine(weights, values):
    return plus(*(times(float(w), v) for w, v in zip(weights, values)))


def sweep(first, nodes, forced, scaled):
    swept = [first]
    for m in range(4):
        inner = combine(QUAD[m], nodes)
        if m:
            inner = plus(inner, times(float(SPACING[m]), minus(swept[m], nodes[m])))
        swept.append(plus(swept[m], times(scaled, inner), forced[m]))
    left = plus(times(scaled, combine(LEFT - 0.5 * np.eye(5)[0], swept)), *forced[:2])
    right = plus(times(scaled, combine(RIGHT - 0.5 * np.eye(5)[2], swept)), *forced[2:])
    return swept, left, right


def chain(start, left, right, gain):
    middle = plus(times(gain, start), left)
    return middle, plus(times(gain, middle), right)


def correct(swept, start, middle, ending):
    deltas = [minus(start, swept[0]), minus(middle, swept[2]), minus(ending, swept[4])]
    return [
        start,
        plus(swept[1], combine(INTERP[1], deltas)),
        middle,
        plus(swept[3], combine(INTERP[3], deltas)),
        ending,
    ]


def march(guesses, forced, scaled, state, final):
    before, first, second = state
    fields = []
    for j, guess in enumerate(guesses):
        gain = 1.0 + 0.5 * scaled[j]
        swept, left, right = sweep(before, [before] + [guess] * 4, forced[j], scaled[j])
        middle, ending = chain(first, left, right, gain)
        nodes = correct(swept, first, middle, ending)
        swept, left, right = sweep(first, nodes, forced[j], scaled[j])
        middle, last = chain(second, left, right, gain)
        if final:
            fields.append(correct(swept, second, middle, last))
        before, first, second = guess, ending, last
    return fields if final else (before, first, second)


def responses(scaled):
    nothing = [0.0] * len(scaled)
    return [
        march(nothing, [[0.0] * 4] * len(scaled), scaled, [float(i == k) for k in range(3)], True)
        for i in range(3)
    ]


def distinct(lo):
    return [(j, m) for j in range(lo) for m in range(5) if j == 0 or m]


def forward_kernel(
    dims, step_ref, init_hbm, guess_hbm, forcing_hbm, parts_hbm, out_ref,
    init_ref, guess_ref, forcing_ref, parts_ref, table_ref, sems, plane_sems,
):
    depth, groups, per, lo, space = dims[:5]
    pieces = lo // depth
    copies = [
        pltpu.make_async_copy(parts_hbm, parts_ref, sems.at[0]),
        pltpu.make_async_copy(init_hbm, init_ref, sems.at[1]),
        pltpu.make_async_copy(guess_hbm.at[0], guess_ref, sems.at[2]),
    ]
    copies += [
        pltpu.make_async_copy(forcing_hbm.at[0, :, d], forcing_ref.at[d], plane_sems.at[d])
        for d in range(depth)
    ]
    for copy in copies:
        copy.start()
    step = step_ref[0]
    width = parts_ref.shape[1]

    for copy in copies:
        copy.wait()
    high, low = parts_ref[0], parts_ref[1]
    table_ref[:width, :width] = high
    table_ref[:width, width:] = high
    table_ref[width:, :width] = low
    table_ref[width:, width:] = jnp.zeros_like(low)

    def transform(planes):
        joined = sine_times(jnp.concatenate(planes, axis=1), table_ref[...])
        half = joined.shape[1] // len(planes)
        return [
            joined[:, i * half : (i + 1) * half].reshape(groups, per, half)
            for i in range(len(planes))
        ]

    def put(field, d, tiles):
        row = (field * depth + d) * per
        out_ref[:, row : row + per, :] = tiles

    starts = transform([init_ref[d] for d in range(depth)])
    mine = lax.axis_index("lo")
    rows = per // pieces
    share = None
    for i in range(lo):
        offset = (i % pieces) * rows
        tile = starts[i // pieces][:, offset : offset + rows]
        share = tile if share is None else jnp.where(mine == i, tile, share)
    base = 5 * depth * per
    out_ref[:, base : base + rows, :] = share
    out_ref[:, base + rows :, :] = jnp.full(
        (groups, out_ref.shape[1] - base - rows, out_ref.shape[2]), step, jnp.float32
    )
    for d, tiles in enumerate(transform([guess_ref[d] for d in range(depth)])):
        put(0, d, tiles)
    for d in range(depth):
        samples = [forcing_ref[d, j] for j in range(5)]
        for m in (0, 2):
            pair = [step * combine(QUAD[k], samples) for k in (m, m + 1)]
            for k, tiles in enumerate(transform(pair)):
                put(1 + m + k, d, tiles)


def source(dims, j, z):
    depth, groups, per, lo, space, cores = dims
    device = z // depth
    return (device % cores * lo + j) * (space // cores) + device // cores, z % depth


def to_modes(dims, got_ref, right_ref, modes_ref, steps_ref):
    depth, groups, per, lo, space, cores = dims
    base = 5 * depth * per + per // (lo // depth)
    count = depth * space
    for j in range(lo):
        columns = []
        for f in range(5):
            tiles = []
            for z in range(count):
                device, d = source(dims, j, z)
                row = (f * depth + d) * per
                tiles.append(got_ref[device, row : row + per, :])
            columns += sine_list(tiles)
        mixed = times_sine(jnp.concatenate(columns, axis=0), right_ref[...])
        modes_ref[j] = mixed.reshape(5, count, per, mixed.shape[1])
        steps_ref[j] = jnp.broadcast_to(
            got_ref[source(dims, j, 0)[0], base : base + 1, :], steps_ref.shape[1:]
        )


def initial_modes(dims, got_ref, right_ref):
    depth, groups, per, lo, space, cores = dims
    pieces = lo // depth
    base = 5 * depth * per
    rows = per // pieces
    tiles = []
    for z in range(depth * space):
        first = (z % depth) * pieces
        parts = [
            got_ref[source(dims, i, z)[0], base : base + rows, :]
            for i in range(first, first + pieces)
        ]
        tiles.append(jnp.concatenate(parts, axis=0))
    mixed = times_sine(jnp.concatenate(sine_list(tiles), axis=0), right_ref[...])
    return mixed.reshape(depth * space, per, mixed.shape[1])


def per_mode(dims, modes_ref, steps_ref, x_ref, y_ref):
    depth, groups, per, lo, space, cores = dims
    device = lax.axis_index("core") * lo + lax.axis_index("lo")
    owner = device * (space // cores) + lax.axis_index("chip")
    plane = x_ref[pl.ds(owner * per, per), :] + y_ref[...]
    steps = [steps_ref[j] for j in range(lo)]
    for z, weight in enumerate(eigen(depth * space)):
        neg = -(plane + float(weight))
        guesses = [modes_ref[j, 0, z] for j in range(lo)]
        forced = [[modes_ref[j, 1 + m, z] for m in range(4)] for j in range(lo)]
        yield z, guesses, forced, [s * neg for s in steps]


def put_fields(dims, fields_of, right_ref, out_ref):
    depth, groups, per, lo, space, cores = dims
    for j in range(lo):
        nodes = range(5) if j == 0 else range(1, 5)
        columns = []
        for m in nodes:
            columns += sine_list(fields_of(j, m))
        mixed = times_sine(jnp.concatenate(columns, axis=0), right_ref[...])
        for k, m in enumerate(nodes):
            places = [(j, m)] + ([(j + 1, 0)] if m == 4 and j + 1 < lo else [])
            for z in range(depth * space):
                first = (k * depth * space + z) * per
                for slot, node in places:
                    device, d = source(dims, slot, z)
                    row = (node * depth + d) * per
                    out_ref[device, row : row + per, :] = mixed[first : first + per]


def first_kernel(
    dims, got_ref, right_ref, x_ref, y_ref, state_ref, modes_ref, steps_ref, start_ref
):
    @pl.when(lax.axis_index("hi") == 0)
    def _():
        to_modes(dims, got_ref, right_ref, modes_ref, steps_ref)
        start_ref[...] = initial_modes(dims, got_ref, right_ref)
        for z, guesses, forced, scaled in per_mode(dims, modes_ref, steps_ref, x_ref, y_ref):
            state = march(guesses, forced, scaled, (start_ref[z],) * 3, False)
            for i in range(3):
                state_ref[i, z] = state[i]


def window_kernel(
    dims, got_ref, modes_in, steps_in, start_ref, right_ref, x_ref, y_ref,
    modes_ref, steps_ref, out_ref, part_ref, unit_ref,
):
    depth, groups, per, lo, space, cores = dims
    head = lax.axis_index("hi") == 0

    @pl.when(head)
    def _():
        for z, guesses, forced, scaled in per_mode(dims, modes_ref, steps_ref, x_ref, y_ref):
            fields = march(guesses, forced, scaled, (start_ref[z],) * 3, True)
            for k, (j, m) in enumerate(distinct(lo)):
                part_ref[k, z] = fields[j][m]
        where = {place: k for k, place in enumerate(distinct(lo))}
        put_fields(
            dims,
            lambda j, m: [part_ref[where[j, m], z] for z in range(depth * space)],
            right_ref,
            out_ref,
        )

    @pl.when(jnp.logical_not(head))
    def _():
        to_modes(dims, got_ref, right_ref, modes_ref, steps_ref)
        for z, guesses, forced, scaled in per_mode(dims, modes_ref, steps_ref, x_ref, y_ref):
            fields = march(guesses, forced, scaled, (0.0,) * 3, True)
            added = responses(scaled)
            for k, (j, m) in enumerate(distinct(lo)):
                if not zero(fields[j][m]):
                    part_ref[k, z] = fields[j][m]
                for i in range(3):
                    if not isinstance(added[i][j][m], float):
                        unit_ref[i, k, z] = added[i][j][m]


def middle_kernel(dims, state_in, modes_ref, steps_ref, came_ref, x_ref, y_ref, state_ref):
    @pl.when(lax.axis_index("hi") > 0)
    def _():
        for z, guesses, forced, scaled in per_mode(dims, modes_ref, steps_ref, x_ref, y_ref):
            came = tuple(came_ref[i, z] for i in range(3))
            state = march(guesses, forced, scaled, came, False)
            for i in range(3):
                state_ref[i, z] = state[i]


def finish_kernel(dims, out_in, part_ref, unit_ref, came_ref, right_ref, out_ref):
    depth, groups, per, lo, space, cores = dims

    @pl.when(lax.axis_index("hi") > 0)
    def _():
        stand = [np.float32(0.5)] * lo
        fields = march(stand, [stand[:1] * 4] * lo, stand, (0.0,) * 3, True)
        added = responses(stand)
        where = {place: k for k, place in enumerate(distinct(lo))}

        def fields_of(j, m):
            k = where[j, m]
            tiles = []
            for z in range(depth * space):
                terms = [] if zero(fields[j][m]) else [part_ref[k, z]]
                for i in range(3):
                    unit = added[i][j][m]
                    if not isinstance(unit, float):
                        unit = unit_ref[i, k, z]
                    terms.append(times(unit, came_ref[i, z]))
                tiles.append(plus(*terms))
            return tiles

        put_fields(dims, fields_of, right_ref, out_ref)


def backward_kernel(dims, got_ref, left_ref, out_hbm, out_ref, sems):
    depth, groups, per = dims[:3]
    width = got_ref.shape[2]
    copies = []
    for i in range(0, 5 * depth, 2):
        pair = jnp.concatenate(
            [
                got_ref[:, k * per : (k + 1) * per, :].reshape(groups * per, width)
                for k in (i, i + 1)
            ],
            axis=1,
        )
        pair = sine_times(pair, left_ref[...])
        for k, plane in ((i, pair[:, :width]), (i + 1, pair[:, width:])):
            out_ref[k] = plane
            copy = pltpu.make_async_copy(
                out_ref.at[k], out_hbm.at[0, k // depth, k % depth], sems.at[k]
            )
            copy.start()
            copies.append(copy)
    for copy in copies:
        copy.wait()


VMEM = pl.BlockSpec(memory_space=pltpu.VMEM)
SMEM = pl.BlockSpec(memory_space=pltpu.SMEM)
HBM = pl.BlockSpec(memory_space=pltpu.HBM)


def in_hbm(value):
    return pltpu.with_memory_space_constraint(value, pltpu.HBM)


def call(kernel, shapes, in_specs, scratch=(), out_spec=VMEM, aliases=None):
    return pl.pallas_call(
        kernel,
        out_shape=[jax.ShapeDtypeStruct(s, jnp.float32) for s in shapes],
        in_specs=in_specs,
        out_specs=[out_spec] * len(shapes),
        scratch_shapes=list(scratch),
        input_output_aliases=aliases or {},
        compiler_params=pltpu.CompilerParams(vmem_limit_bytes=12 * 2**20),
    )


def body(initial, start_guess, forcing, step_size):
    depth, width_x, width_y = initial.shape
    hi, lo, chips, cores = (lax.axis_size(a) for a in ("hi", "lo", "chip", "core"))
    space = chips * cores
    groups = space * lo
    per = width_x // groups
    dims = (depth, groups, per, lo, space, cores)
    count = depth * space
    parts = jnp.asarray(sine_parts(width_x))
    right = jnp.asarray(right_table(width_y))
    left = jnp.asarray(left_table(width_x))
    x_weights = jnp.asarray(
        np.broadcast_to(eigen(width_x)[:, None], (width_x, width_y)).astype(np.float32)
    )
    y_weights = jnp.asarray(eigen(width_y)[None, :].astype(np.float32))
    tile = (per, width_y)
    plane = (width_x, width_y)
    bind = functools.partial

    rows = 5 * depth * per
    (send,) = call(
        bind(forward_kernel, dims),
        [(groups, rows + TILE, width_y)],
        [SMEM] + [HBM] * 4,
        [
            pltpu.VMEM((depth, *plane), jnp.float32),
            pltpu.VMEM((depth, *plane), jnp.float32),
            pltpu.VMEM((depth, 5, *plane), jnp.float32),
            pltpu.VMEM(parts.shape, parts.dtype),
            pltpu.VMEM(left.shape, left.dtype),
            pltpu.SemaphoreType.DMA((3,)),
            pltpu.SemaphoreType.DMA((depth,)),
        ],
    )(step_size, *(in_hbm(a) for a in (initial, start_guess, forcing, parts)))
    members = ("core", "lo", "chip")
    got = lax.all_to_all(send, members, 0, 0, tiled=True)
    state_shape, modes_shape, steps_shape = (3, count, *tile), (lo, 5, count, *tile), (lo, *tile)
    state, modes, steps, start = call(
        bind(first_kernel, dims),
        [state_shape, modes_shape, steps_shape, (count, *tile)],
        [VMEM] * 4,
    )(got, right, x_weights, y_weights)
    onward = [(i, i + 1) for i in range(hi - 1)]
    came = lax.ppermute(state, "hi", onward)
    kinds = len(distinct(lo))
    modes, steps, send, part, unit = call(
        bind(window_kernel, dims),
        [
            modes_shape,
            steps_shape,
            (groups, rows, width_y),
            (kinds, count, *tile),
            (3, kinds, count, *tile),
        ],
        [VMEM] * 7,
        aliases={1: 0, 2: 1},
    )(got, modes, steps, start, right, x_weights, y_weights)
    for _ in range(hi - 2):
        (state,) = call(bind(middle_kernel, dims), [state_shape], [VMEM] * 6, aliases={0: 0})(
            state, modes, steps, came, x_weights, y_weights
        )
        came = lax.ppermute(state, "hi", onward)
    (send,) = call(
        bind(finish_kernel, dims), [(groups, rows, width_y)], [VMEM] * 5, aliases={0: 0}
    )(send, part, unit, came, right)
    got = lax.all_to_all(send, members, 0, 0, tiled=True)
    (fields,) = call(
        bind(backward_kernel, dims),
        [(1, 5, depth, width_x, width_y)],
        [VMEM] * 2,
        [
            pltpu.VMEM((5 * depth, *plane), jnp.float32),
            pltpu.SemaphoreType.DMA((5 * depth,)),
        ],
        HBM,
    )(got, left)
    return fields


def solution(mesh):
    steps, space = mesh.devices.shape
    cores = 2 if space % 2 == 0 else 1
    time, slabs = ("hi", "lo"), ("chip", "core")
    specs = (P(slabs), P(time, slabs), P(time, None, slabs), P(time))

    def run(initial, start_guess, forcing, step_size):
        width = initial.shape[1]
        lo = max(
            d for d in range(1, steps + 1) if steps % d == 0 and width % (TILE * d * space) == 0
        )
        shape = (steps // lo, lo, space // cores, cores)
        whole = Mesh(mesh.devices.reshape(shape), time + slabs)
        return jax.shard_map(
            body, mesh=whole, in_specs=specs, out_specs=P(time, None, slabs), check_vma=False
        )(initial, start_guess, forcing, step_size)

    return run
```

```python
import functools
import math

import jax
import jax.numpy as jnp
import numpy as np
from jax import lax
from jax.experimental import pallas as pl
from jax.experimental.pallas import tpu as pltpu
from jax.sharding import Mesh
from jax.sharding import PartitionSpec as P

TILE = 8
COST = 10**10


def node_tables():
    radical = math.sqrt(3.0 / 7.0)
    node_times = [0.0, (1.0 - radical) / 2.0, 0.5, (1.0 + radical) / 2.0, 1.0]
    integrals = np.zeros((4, 5))
    for column in range(5):
        coeffs = [1.0]
        for other_index in range(5):
            if other_index == column:
                continue
            other_time = node_times[other_index]
            scaling = node_times[column] - other_time
            grown = [0.0] * (len(coeffs) + 1)
            for exponent in range(len(coeffs)):
                grown[exponent + 1] += coeffs[exponent] / scaling
                grown[exponent] -= coeffs[exponent] * other_time / scaling
            coeffs = grown
        for section in range(4):
            integrals[section, column] = sum(
                coeffs[exponent]
                * (node_times[section + 1] ** (exponent + 1) - node_times[section] ** (exponent + 1))
                / (exponent + 1)
                for exponent in range(len(coeffs))
            )
    coarse = [0.0, 0.5, 1.0]
    interp = np.zeros((5, 3))
    for column in range(3):
        for section in range(5):
            weight = 1.0
            for other_index in range(3):
                if other_index != column:
                    weight = (
                        weight
                        * (node_times[section] - coarse[other_index])
                        / (coarse[column] - coarse[other_index])
                    )
            interp[section, column] = weight
    return (np.array(node_times), integrals, interp)


TIMES, QUAD, INTERP = node_tables()
SPACING = np.diff(TIMES)
LEFT = QUAD[0] + QUAD[1]
RIGHT = QUAD[2] + QUAD[3]


def sine(length):
    index = np.arange(1, length + 1)
    return math.sqrt(2.0 / (length + 1)) * np.sin(math.pi / (length + 1) * np.outer(index, index))


def eigen(length):
    return 2.0 - 2.0 * np.cos(math.pi / (length + 1) * np.arange(1, length + 1))


def sine_parts(length):
    matrix = sine(length)
    high = matrix.astype(jnp.bfloat16)
    low = (matrix - high.astype(np.float64)).astype(jnp.bfloat16)
    return np.stack([high, low])


def right_table(length):
    high, low = sine_parts(length)
    return np.block([[high, low], [high, np.zeros_like(high)]])


def left_table(length):
    high, low = sine_parts(length)
    return np.block([[high, high], [low, np.zeros_like(high)]])


def split(value):
    high = value.astype(jnp.bfloat16)
    return high, (value - high.astype(jnp.float32)).astype(jnp.bfloat16)


def times_sine(value, table):
    width = value.shape[-1]
    both = jnp.dot(
        jnp.concatenate(split(value), axis=1), table, preferred_element_type=jnp.float32
    )
    return both[:, :width] + both[:, width:]


def sine_times(value, table):
    width = value.shape[0]
    both = jnp.dot(
        table, jnp.concatenate(split(value), axis=0), preferred_element_type=jnp.float32
    )
    return both[:width] + both[width:]


def sine_list(values):
    count = len(values)
    matrix = sine(count)
    half = count // 2
    even = [values[i] + values[count - 1 - i] for i in range(half)]
    odd = [values[i] - values[count - 1 - i] for i in range(half)]
    middle = [values[half]] if count % 2 else []
    result = []
    for k in range(count):
        terms = even + middle if k % 2 == 0 else odd
        result.append(sum(float(matrix[k, i]) * term for i, term in enumerate(terms)))
    return result


def zero(value):
    return isinstance(value, float) and value == 0.0


def plus(*values):
    values = [v for v in values if not zero(v)]
    return sum(values[1:], values[0]) if values else 0.0


def times(factor, value):
    return 0.0 if zero(factor) or zero(value) else factor * value


def minus(value, other):
    return value if zero(other) else plus(value, -other)


def combine(weights, values):
    return plus(*(times(float(w), v) for w, v in zip(weights, values)))


def sweep(first, nodes, forced, scaled):
    swept = [first]
    for m in range(4):
        inner = combine(QUAD[m], nodes)
        if m:
            inner = plus(inner, times(float(SPACING[m]), minus(swept[m], nodes[m])))
        swept.append(plus(swept[m], times(scaled, inner), forced[m]))
    left = plus(times(scaled, combine(LEFT - 0.5 * np.eye(5)[0], swept)), *forced[:2])
    right = plus(times(scaled, combine(RIGHT - 0.5 * np.eye(5)[2], swept)), *forced[2:])
    return swept, left, right


def chain(start, left, right, gain):
    middle = plus(times(gain, start), left)
    return middle, plus(times(gain, middle), right)


def correct(swept, start, middle, ending):
    deltas = [minus(start, swept[0]), minus(middle, swept[2]), minus(ending, swept[4])]
    return [
        start,
        plus(swept[1], combine(INTERP[1], deltas)),
        middle,
        plus(swept[3], combine(INTERP[3], deltas)),
        ending,
    ]


def march(guesses, forced, scaled, state, final):
    before, first, second = state
    fields = []
    for j, guess in enumerate(guesses):
        gain = 1.0 + 0.5 * scaled[j]
        swept, left, right = sweep(before, [before] + [guess] * 4, forced[j], scaled[j])
        middle, ending = chain(first, left, right, gain)
        nodes = correct(swept, first, middle, ending)
        swept, left, right = sweep(first, nodes, forced[j], scaled[j])
        middle, last = chain(second, left, right, gain)
        if final:
            fields.append(correct(swept, second, middle, last))
        before, first, second = guess, ending, last
    return fields if final else (before, first, second)


def responses(scaled):
    nothing = [0.0] * len(scaled)
    return [
        march(nothing, [[0.0] * 4] * len(scaled), scaled, [float(i == k) for k in range(3)], True)
        for i in range(3)
    ]


def distinct(lo):
    return [(j, m) for j in range(lo) for m in range(5) if j == 0 or m]


def blank_kernel(out_ref):
    out_ref[...] = jnp.zeros(out_ref.shape, out_ref.dtype)


def forward_kernel(
    dims, step_ref, init_ref, guess_ref, forcing_ref, parts_ref, blank_ref, out_ref, table_ref
):
    depth, groups, per, lo, space = dims[:5]
    pieces = lo // depth
    width = parts_ref.shape[1]
    high, low = parts_ref[0], parts_ref[1]
    table_ref[:width, :width] = high
    table_ref[:width, width:] = high
    table_ref[width:, :width] = low
    table_ref[width:, width:] = blank_ref[...]

    def transform(planes):
        joined = sine_times(jnp.concatenate(planes, axis=1), table_ref[...])
        half = joined.shape[1] // len(planes)
        return [
            joined[:, i * half : (i + 1) * half].reshape(groups, per, half)
            for i in range(len(planes))
        ]

    def put(field, d, tiles):
        row = (field * depth + d) * per
        out_ref[:, row : row + per, :] = tiles

    starts = transform([init_ref[d] for d in range(depth)])
    mine = lax.axis_index("lo")
    rows = per // pieces
    share = None
    for i in range(lo):
        offset = (i % pieces) * rows
        tile = starts[i // pieces][:, offset : offset + rows]
        share = tile if share is None else jnp.where(mine == i, tile, share)
    step = step_ref[0]
    base = 5 * depth * per
    out_ref[:, base : base + rows, :] = share
    out_ref[:, base + rows :, :] = jnp.full(
        (groups, out_ref.shape[1] - base - rows, out_ref.shape[2]), step, jnp.float32
    )
    for d, tiles in enumerate(transform([guess_ref[0, d] for d in range(depth)])):
        put(0, d, tiles)
    for d in range(depth):
        samples = [forcing_ref[0, j, d] for j in range(5)]
        for m in (0, 2):
            pair = [step * combine(QUAD[k], samples) for k in (m, m + 1)]
            for k, tiles in enumerate(transform(pair)):
                put(1 + m + k, d, tiles)


def source(dims, j, z):
    depth, groups, per, lo, space, cores = dims
    device = z // depth
    return (device % cores * lo + j) * (space // cores) + device // cores, z % depth


def to_modes(dims, got_ref, right_ref, modes_ref, steps_ref):
    depth, groups, per, lo, space, cores = dims
    base = 5 * depth * per + per // (lo // depth)
    count = depth * space
    for j in range(lo):
        columns = []
        for f in range(5):
            tiles = []
            for z in range(count):
                device, d = source(dims, j, z)
                row = (f * depth + d) * per
                tiles.append(got_ref[device, row : row + per, :])
            columns += sine_list(tiles)
        mixed = times_sine(jnp.concatenate(columns, axis=0), right_ref[...])
        modes_ref[j] = mixed.reshape(5, count, per, mixed.shape[1])
        steps_ref[j] = jnp.broadcast_to(
            got_ref[source(dims, j, 0)[0], base : base + 1, :], steps_ref.shape[1:]
        )


def initial_modes(dims, got_ref, right_ref):
    depth, groups, per, lo, space, cores = dims
    pieces = lo // depth
    base = 5 * depth * per
    rows = per // pieces
    tiles = []
    for z in range(depth * space):
        first = (z % depth) * pieces
        parts = [
            got_ref[source(dims, i, z)[0], base : base + rows, :]
            for i in range(first, first + pieces)
        ]
        tiles.append(jnp.concatenate(parts, axis=0))
    mixed = times_sine(jnp.concatenate(sine_list(tiles), axis=0), right_ref[...])
    return mixed.reshape(depth * space, per, mixed.shape[1])


def per_mode(dims, modes_ref, steps_ref, x_ref, y_ref):
    depth, groups, per, lo, space, cores = dims
    device = lax.axis_index("core") * lo + lax.axis_index("lo")
    owner = device * (space // cores) + lax.axis_index("chip")
    plane = x_ref[pl.ds(owner * per, per), :] + y_ref[...]
    steps = [steps_ref[j] for j in range(lo)]
    for z, weight in enumerate(eigen(depth * space)):
        neg = -(plane + float(weight))
        guesses = [modes_ref[j, 0, z] for j in range(lo)]
        forced = [[modes_ref[j, 1 + m, z] for m in range(4)] for j in range(lo)]
        yield z, guesses, forced, [s * neg for s in steps]


def put_fields(dims, fields_of, right_ref, out_ref):
    depth, groups, per, lo, space, cores = dims
    for j in range(lo):
        nodes = range(5) if j == 0 else range(1, 5)
        columns = []
        for m in nodes:
            columns += sine_list(fields_of(j, m))
        mixed = times_sine(jnp.concatenate(columns, axis=0), right_ref[...])
        for k, m in enumerate(nodes):
            places = [(j, m)] + ([(j + 1, 0)] if m == 4 and j + 1 < lo else [])
            for z in range(depth * space):
                first = (k * depth * space + z) * per
                for slot, node in places:
                    device, d = source(dims, slot, z)
                    row = (node * depth + d) * per
                    out_ref[device, row : row + per, :] = mixed[first : first + per]


def first_kernel(
    dims, got_ref, right_ref, x_ref, y_ref, state_ref, modes_ref, steps_ref, start_ref
):
    @pl.when(lax.axis_index("hi") == 0)
    def _():
        to_modes(dims, got_ref, right_ref, modes_ref, steps_ref)
        start_ref[...] = initial_modes(dims, got_ref, right_ref)
        for z, guesses, forced, scaled in per_mode(dims, modes_ref, steps_ref, x_ref, y_ref):
            state = march(guesses, forced, scaled, (start_ref[z],) * 3, False)
            for i in range(3):
                state_ref[i, z] = state[i]


def window_kernel(
    dims, got_ref, modes_in, steps_in, start_ref, right_ref, x_ref, y_ref,
    modes_ref, steps_ref, out_ref, part_ref, unit_ref,
):
    depth, groups, per, lo, space, cores = dims
    head = lax.axis_index("hi") == 0

    @pl.when(head)
    def _():
        for z, guesses, forced, scaled in per_mode(dims, modes_ref, steps_ref, x_ref, y_ref):
            fields = march(guesses, forced, scaled, (start_ref[z],) * 3, True)
            for k, (j, m) in enumerate(distinct(lo)):
                part_ref[k, z] = fields[j][m]
        where = {place: k for k, place in enumerate(distinct(lo))}
        put_fields(
            dims,
            lambda j, m: [part_ref[where[j, m], z] for z in range(depth * space)],
            right_ref,
            out_ref,
        )

    @pl.when(jnp.logical_not(head))
    def _():
        to_modes(dims, got_ref, right_ref, modes_ref, steps_ref)
        for z, guesses, forced, scaled in per_mode(dims, modes_ref, steps_ref, x_ref, y_ref):
            fields = march(guesses, forced, scaled, (0.0,) * 3, True)
            added = responses(scaled)
            for k, (j, m) in enumerate(distinct(lo)):
                if not zero(fields[j][m]):
                    part_ref[k, z] = fields[j][m]
                for i in range(3):
                    if not isinstance(added[i][j][m], float):
                        unit_ref[i, k, z] = added[i][j][m]


def middle_kernel(dims, state_in, modes_ref, steps_ref, came_ref, x_ref, y_ref, state_ref):
    @pl.when(lax.axis_index("hi") > 0)
    def _():
        for z, guesses, forced, scaled in per_mode(dims, modes_ref, steps_ref, x_ref, y_ref):
            came = tuple(came_ref[i, z] for i in range(3))
            state = march(guesses, forced, scaled, came, False)
            for i in range(3):
                state_ref[i, z] = state[i]


def finish_kernel(dims, out_in, part_ref, unit_ref, came_ref, right_ref, out_ref):
    depth, groups, per, lo, space, cores = dims

    @pl.when(lax.axis_index("hi") > 0)
    def _():
        stand = [np.float32(0.5)] * lo
        fields = march(stand, [stand[:1] * 4] * lo, stand, (0.0,) * 3, True)
        added = responses(stand)
        where = {place: k for k, place in enumerate(distinct(lo))}

        def fields_of(j, m):
            k = where[j, m]
            tiles = []
            for z in range(depth * space):
                terms = [] if zero(fields[j][m]) else [part_ref[k, z]]
                for i in range(3):
                    unit = added[i][j][m]
                    if not isinstance(unit, float):
                        unit = unit_ref[i, k, z]
                    terms.append(times(unit, came_ref[i, z]))
                tiles.append(plus(*terms))
            return tiles

        put_fields(dims, fields_of, right_ref, out_ref)


def backward_kernel(dims, got_ref, left_ref, out_hbm, out_ref, sems):
    depth, groups, per = dims[:3]
    width = got_ref.shape[2]
    copies = []
    for i in range(0, 5 * depth, 2):
        pair = jnp.concatenate(
            [
                got_ref[:, k * per : (k + 1) * per, :].reshape(groups * per, width)
                for k in (i, i + 1)
            ],
            axis=1,
        )
        pair = sine_times(pair, left_ref[...])
        for k, plane in ((i, pair[:, :width]), (i + 1, pair[:, width:])):
            out_ref[k] = plane
            copy = pltpu.make_async_copy(
                out_ref.at[k], out_hbm.at[0, k // depth, k % depth], sems.at[k]
            )
            copy.start()
            copies.append(copy)
    for copy in copies:
        copy.wait()


VMEM = pl.BlockSpec(memory_space=pltpu.VMEM)
SMEM = pl.BlockSpec(memory_space=pltpu.SMEM)
HBM = pl.BlockSpec(memory_space=pltpu.HBM)


def call(kernel, shapes, in_specs, scratch=(), out_spec=VMEM, aliases=None):
    return pl.pallas_call(
        kernel,
        out_shape=[jax.ShapeDtypeStruct(s, jnp.float32) for s in shapes],
        in_specs=in_specs,
        out_specs=[out_spec] * len(shapes),
        scratch_shapes=list(scratch),
        input_output_aliases=aliases or {},
        compiler_params=pltpu.CompilerParams(vmem_limit_bytes=12 * 2**20),
    )


def body(initial, start_guess, forcing, step_size):
    depth, width_x, width_y = initial.shape
    hi, lo, chips, cores = (lax.axis_size(a) for a in ("hi", "lo", "chip", "core"))
    space = chips * cores
    groups = space * lo
    per = width_x // groups
    dims = (depth, groups, per, lo, space, cores)
    count = depth * space
    parts = jnp.asarray(sine_parts(width_x))
    right = jnp.asarray(right_table(width_y))
    left = jnp.asarray(left_table(width_x))
    x_weights = jnp.asarray(
        np.broadcast_to(eigen(width_x)[:, None], (width_x, width_y)).astype(np.float32)
    )
    y_weights = jnp.asarray(eigen(width_y)[None, :].astype(np.float32))
    tile = (per, width_y)
    plane = (width_x, width_y)
    bind = functools.partial

    rows = 5 * depth * per
    extra = -(-(per // (lo // depth) + 1) // TILE) * TILE
    blank = pl.pallas_call(
        blank_kernel,
        out_shape=jax.ShapeDtypeStruct((width_x, width_x), parts.dtype),
        out_specs=VMEM,
        cost_estimate=pl.CostEstimate(flops=COST, bytes_accessed=COST, transcendentals=0),
        compiler_params=pltpu.CompilerParams(vmem_limit_bytes=2**20),
    )()
    (send,) = call(
        bind(forward_kernel, dims),
        [(groups, rows + extra, width_y)],
        [SMEM] + [VMEM] * 5,
        [pltpu.VMEM(left.shape, left.dtype)],
    )(step_size, initial, start_guess, forcing, parts, blank)
    members = ("core", "lo", "chip")
    got = lax.all_to_all(send, members, 0, 0, tiled=True)
    state_shape, modes_shape, steps_shape = (3, count, *tile), (lo, 5, count, *tile), (lo, *tile)
    state, modes, steps, start = call(
        bind(first_kernel, dims),
        [state_shape, modes_shape, steps_shape, (count, *tile)],
        [VMEM] * 4,
    )(got, right, x_weights, y_weights)
    onward = [(i, i + 1) for i in range(hi - 1)]
    came = lax.ppermute(state, "hi", onward)
    kinds = len(distinct(lo))
    modes, steps, send, part, unit = call(
        bind(window_kernel, dims),
        [
            modes_shape,
            steps_shape,
            (groups, rows, width_y),
            (kinds, count, *tile),
            (3, kinds, count, *tile),
        ],
        [VMEM] * 7,
        aliases={1: 0, 2: 1},
    )(got, modes, steps, start, right, x_weights, y_weights)
    for _ in range(hi - 2):
        (state,) = call(bind(middle_kernel, dims), [state_shape], [VMEM] * 6, aliases={0: 0})(
            state, modes, steps, came, x_weights, y_weights
        )
        came = lax.ppermute(state, "hi", onward)
    (send,) = call(
        bind(finish_kernel, dims), [(groups, rows, width_y)], [VMEM] * 5, aliases={0: 0}
    )(send, part, unit, came, right)
    got = lax.all_to_all(send, members, 0, 0, tiled=True)
    (fields,) = call(
        bind(backward_kernel, dims),
        [(1, 5, depth, width_x, width_y)],
        [VMEM] * 2,
        [
            pltpu.VMEM((5 * depth, *plane), jnp.float32),
            pltpu.SemaphoreType.DMA((5 * depth,)),
        ],
        HBM,
    )(got, left)
    return fields


def solution(mesh):
    steps, space = mesh.devices.shape
    cores = 2 if space % 2 == 0 else 1
    time, slabs = ("hi", "lo"), ("chip", "core")
    specs = (P(slabs), P(time, slabs), P(time, None, slabs), P(time))

    def run(initial, start_guess, forcing, step_size):
        width = initial.shape[1]
        lo = max(
            d for d in range(1, steps + 1) if steps % d == 0 and width % (TILE * d * space) == 0
        )
        shape = (steps // lo, lo, space // cores, cores)
        whole = Mesh(mesh.devices.reshape(shape), time + slabs)
        return jax.shard_map(
            body, mesh=whole, in_specs=specs, out_specs=P(time, None, slabs), check_vma=False
        )(initial, start_guess, forcing, step_size)

    return run
```

```python
import functools
import math

import jax
import jax.numpy as jnp
import numpy as np
from jax import lax
from jax.experimental import pallas as pl
from jax.experimental.pallas import tpu as pltpu
from jax.sharding import Mesh
from jax.sharding import PartitionSpec as P

TILE = 8
COST = 10**10


def node_tables():
    radical = math.sqrt(3.0 / 7.0)
    node_times = [0.0, (1.0 - radical) / 2.0, 0.5, (1.0 + radical) / 2.0, 1.0]
    integrals = np.zeros((4, 5))
    for column in range(5):
        coeffs = [1.0]
        for other_index in range(5):
            if other_index == column:
                continue
            other_time = node_times[other_index]
            scaling = node_times[column] - other_time
            grown = [0.0] * (len(coeffs) + 1)
            for exponent in range(len(coeffs)):
                grown[exponent + 1] += coeffs[exponent] / scaling
                grown[exponent] -= coeffs[exponent] * other_time / scaling
            coeffs = grown
        for section in range(4):
            integrals[section, column] = sum(
                coeffs[exponent]
                * (node_times[section + 1] ** (exponent + 1) - node_times[section] ** (exponent + 1))
                / (exponent + 1)
                for exponent in range(len(coeffs))
            )
    coarse = [0.0, 0.5, 1.0]
    interp = np.zeros((5, 3))
    for column in range(3):
        for section in range(5):
            weight = 1.0
            for other_index in range(3):
                if other_index != column:
                    weight = (
                        weight
                        * (node_times[section] - coarse[other_index])
                        / (coarse[column] - coarse[other_index])
                    )
            interp[section, column] = weight
    return (np.array(node_times), integrals, interp)


TIMES, QUAD, INTERP = node_tables()
SPACING = np.diff(TIMES)
LEFT = QUAD[0] + QUAD[1]
RIGHT = QUAD[2] + QUAD[3]


def sine(length):
    index = np.arange(1, length + 1)
    return math.sqrt(2.0 / (length + 1)) * np.sin(math.pi / (length + 1) * np.outer(index, index))


def eigen(length):
    return 2.0 - 2.0 * np.cos(math.pi / (length + 1) * np.arange(1, length + 1))


def sine_parts(length):
    matrix = sine(length)
    high = matrix.astype(jnp.bfloat16)
    low = (matrix - high.astype(np.float64)).astype(jnp.bfloat16)
    return np.stack([high, low])


def right_table(length):
    high, low = sine_parts(length)
    return np.block([[high, low], [high, np.zeros_like(high)]])


def left_table(length):
    high, low = sine_parts(length)
    return np.block([[high, high], [low, np.zeros_like(high)]])


def split(value):
    high = value.astype(jnp.bfloat16)
    return high, (value - high.astype(jnp.float32)).astype(jnp.bfloat16)


def times_sine(value, table):
    width = value.shape[-1]
    both = jnp.dot(
        jnp.concatenate(split(value), axis=1), table, preferred_element_type=jnp.float32
    )
    return both[:, :width] + both[:, width:]


def sine_times(value, table):
    width = value.shape[0]
    both = jnp.dot(
        table, jnp.concatenate(split(value), axis=0), preferred_element_type=jnp.float32
    )
    return both[:width] + both[width:]


def sine_list(values):
    count = len(values)
    matrix = sine(count)
    half = count // 2
    even = [values[i] + values[count - 1 - i] for i in range(half)]
    odd = [values[i] - values[count - 1 - i] for i in range(half)]
    middle = [values[half]] if count % 2 else []
    result = []
    for k in range(count):
        terms = even + middle if k % 2 == 0 else odd
        result.append(sum(float(matrix[k, i]) * term for i, term in enumerate(terms)))
    return result


def zero(value):
    return isinstance(value, float) and value == 0.0


def plus(*values):
    values = [v for v in values if not zero(v)]
    return sum(values[1:], values[0]) if values else 0.0


def times(factor, value):
    return 0.0 if zero(factor) or zero(value) else factor * value


def minus(value, other):
    return value if zero(other) else plus(value, -other)


def combine(weights, values):
    return plus(*(times(float(w), v) for w, v in zip(weights, values)))


def sweep(first, nodes, forced, scaled):
    swept = [first]
    for m in range(4):
        inner = combine(QUAD[m], nodes)
        if m:
            inner = plus(inner, times(float(SPACING[m]), minus(swept[m], nodes[m])))
        swept.append(plus(swept[m], times(scaled, inner), forced[m]))
    left = plus(times(scaled, combine(LEFT - 0.5 * np.eye(5)[0], swept)), *forced[:2])
    right = plus(times(scaled, combine(RIGHT - 0.5 * np.eye(5)[2], swept)), *forced[2:])
    return swept, left, right


def chain(start, left, right, gain):
    middle = plus(times(gain, start), left)
    return middle, plus(times(gain, middle), right)


def correct(swept, start, middle, ending):
    deltas = [minus(start, swept[0]), minus(middle, swept[2]), minus(ending, swept[4])]
    return [
        start,
        plus(swept[1], combine(INTERP[1], deltas)),
        middle,
        plus(swept[3], combine(INTERP[3], deltas)),
        ending,
    ]


def march(guesses, forced, scaled, state, final):
    before, first, second = state
    fields = []
    for j, guess in enumerate(guesses):
        gain = 1.0 + 0.5 * scaled[j]
        swept, left, right = sweep(before, [before] + [guess] * 4, forced[j], scaled[j])
        middle, ending = chain(first, left, right, gain)
        nodes = correct(swept, first, middle, ending)
        swept, left, right = sweep(first, nodes, forced[j], scaled[j])
        middle, last = chain(second, left, right, gain)
        if final:
            fields.append(correct(swept, second, middle, last))
        before, first, second = guess, ending, last
    return fields if final else (before, first, second)


def responses(scaled):
    nothing = [0.0] * len(scaled)
    return [
        march(nothing, [[0.0] * 4] * len(scaled), scaled, [float(i == k) for k in range(3)], True)
        for i in range(3)
    ]


def distinct(lo):
    return [(j, m) for j in range(lo) for m in range(5) if j == 0 or m]


def blank_kernel(out_ref):
    out_ref[...] = jnp.zeros(out_ref.shape, out_ref.dtype)


def forward_kernel(
    dims, step_ref, init_ref, guess_ref, forcing_ref, parts_ref, blank_ref, out_ref, table_ref
):
    depth, groups, per, lo, space = dims[:5]
    pieces = lo // depth
    width = parts_ref.shape[1]
    high, low = parts_ref[0], parts_ref[1]
    table_ref[:width, :width] = high
    table_ref[:width, width:] = high
    table_ref[width:, :width] = low
    table_ref[width:, width:] = blank_ref[...]

    def transform(planes):
        joined = sine_times(jnp.concatenate(planes, axis=1), table_ref[...])
        half = joined.shape[1] // len(planes)
        return [
            joined[:, i * half : (i + 1) * half].reshape(groups, per, half)
            for i in range(len(planes))
        ]

    def put(field, d, tiles):
        row = (field * depth + d) * per
        out_ref[:, row : row + per, :] = tiles

    starts = transform([init_ref[d] for d in range(depth)])
    mine = lax.axis_index("lo")
    rows = per // pieces
    share = None
    for i in range(lo):
        offset = (i % pieces) * rows
        tile = starts[i // pieces][:, offset : offset + rows]
        share = tile if share is None else jnp.where(mine == i, tile, share)
    step = step_ref[0]
    base = 5 * depth * per
    out_ref[:, base : base + rows, :] = share
    out_ref[:, base + rows :, :] = jnp.full(
        (groups, out_ref.shape[1] - base - rows, out_ref.shape[2]), step, jnp.float32
    )
    for d, tiles in enumerate(transform([guess_ref[0, d] for d in range(depth)])):
        put(0, d, tiles)
    for d in range(depth):
        samples = [forcing_ref[0, j, d] for j in range(5)]
        for m in (0, 2):
            pair = [step * combine(QUAD[k], samples) for k in (m, m + 1)]
            for k, tiles in enumerate(transform(pair)):
                put(1 + m + k, d, tiles)


def source(dims, j, z):
    depth, groups, per, lo, space, cores = dims
    device = z // depth
    return (device % cores * lo + j) * (space // cores) + device // cores, z % depth


def to_modes(dims, got_ref, right_ref, modes_ref, steps_ref):
    depth, groups, per, lo, space, cores = dims
    base = 5 * depth * per + per // (lo // depth)
    count = depth * space
    for j in range(lo):
        columns = []
        for f in range(5):
            tiles = []
            for z in range(count):
                device, d = source(dims, j, z)
                row = (f * depth + d) * per
                tiles.append(got_ref[device, row : row + per, :])
            columns += sine_list(tiles)
        mixed = times_sine(jnp.concatenate(columns, axis=0), right_ref[...])
        modes_ref[j] = mixed.reshape(5, count, per, mixed.shape[1])
        steps_ref[j] = jnp.broadcast_to(
            got_ref[source(dims, j, 0)[0], base : base + 1, :], steps_ref.shape[1:]
        )


def initial_modes(dims, got_ref, right_ref):
    depth, groups, per, lo, space, cores = dims
    pieces = lo // depth
    base = 5 * depth * per
    rows = per // pieces
    tiles = []
    for z in range(depth * space):
        first = (z % depth) * pieces
        parts = [
            got_ref[source(dims, i, z)[0], base : base + rows, :]
            for i in range(first, first + pieces)
        ]
        tiles.append(jnp.concatenate(parts, axis=0))
    mixed = times_sine(jnp.concatenate(sine_list(tiles), axis=0), right_ref[...])
    return mixed.reshape(depth * space, per, mixed.shape[1])


def per_mode(dims, modes_ref, steps_ref, x_ref, y_ref):
    depth, groups, per, lo, space, cores = dims
    device = lax.axis_index("core") * lo + lax.axis_index("lo")
    owner = device * (space // cores) + lax.axis_index("chip")
    plane = x_ref[pl.ds(owner * per, per), :] + y_ref[...]
    steps = [steps_ref[j] for j in range(lo)]
    for z, weight in enumerate(eigen(depth * space)):
        neg = -(plane + float(weight))
        guesses = [modes_ref[j, 0, z] for j in range(lo)]
        forced = [[modes_ref[j, 1 + m, z] for m in range(4)] for j in range(lo)]
        yield z, guesses, forced, [s * neg for s in steps]


def put_fields(dims, fields_of, right_ref, out_ref):
    depth, groups, per, lo, space, cores = dims
    for j in range(lo):
        nodes = range(5) if j == 0 else range(1, 5)
        columns = []
        for m in nodes:
            columns += sine_list(fields_of(j, m))
        mixed = times_sine(jnp.concatenate(columns, axis=0), right_ref[...])
        for k, m in enumerate(nodes):
            places = [(j, m)] + ([(j + 1, 0)] if m == 4 and j + 1 < lo else [])
            for z in range(depth * space):
                first = (k * depth * space + z) * per
                for slot, node in places:
                    device, d = source(dims, slot, z)
                    row = (node * depth + d) * per
                    out_ref[device, row : row + per, :] = mixed[first : first + per]


def first_kernel(
    dims, got_ref, right_ref, x_ref, y_ref, state_ref, modes_ref, steps_ref, start_ref
):
    @pl.when(lax.axis_index("hi") == 0)
    def _():
        to_modes(dims, got_ref, right_ref, modes_ref, steps_ref)
        start_ref[...] = initial_modes(dims, got_ref, right_ref)
        for z, guesses, forced, scaled in per_mode(dims, modes_ref, steps_ref, x_ref, y_ref):
            state = march(guesses, forced, scaled, (start_ref[z],) * 3, False)
            for i in range(3):
                state_ref[i, z] = state[i]


def window_kernel(
    dims, got_ref, modes_in, steps_in, start_ref, right_ref, x_ref, y_ref,
    modes_ref, steps_ref, out_ref, part_ref, unit_ref,
):
    depth, groups, per, lo, space, cores = dims
    head = lax.axis_index("hi") == 0

    @pl.when(head)
    def _():
        for z, guesses, forced, scaled in per_mode(dims, modes_ref, steps_ref, x_ref, y_ref):
            fields = march(guesses, forced, scaled, (start_ref[z],) * 3, True)
            for k, (j, m) in enumerate(distinct(lo)):
                part_ref[k, z] = fields[j][m]
        where = {place: k for k, place in enumerate(distinct(lo))}
        put_fields(
            dims,
            lambda j, m: [part_ref[where[j, m], z] for z in range(depth * space)],
            right_ref,
            out_ref,
        )

    @pl.when(jnp.logical_not(head))
    def _():
        to_modes(dims, got_ref, right_ref, modes_ref, steps_ref)
        for z, guesses, forced, scaled in per_mode(dims, modes_ref, steps_ref, x_ref, y_ref):
            fields = march(guesses, forced, scaled, (0.0,) * 3, True)
            added = responses(scaled)
            for k, (j, m) in enumerate(distinct(lo)):
                if not zero(fields[j][m]):
                    part_ref[k, z] = fields[j][m]
                for i in range(3):
                    if not isinstance(added[i][j][m], float):
                        unit_ref[i, k, z] = added[i][j][m]


def middle_kernel(dims, state_in, modes_ref, steps_ref, came_ref, x_ref, y_ref, state_ref):
    @pl.when(lax.axis_index("hi") > 0)
    def _():
        for z, guesses, forced, scaled in per_mode(dims, modes_ref, steps_ref, x_ref, y_ref):
            came = tuple(came_ref[i, z] for i in range(3))
            state = march(guesses, forced, scaled, came, False)
            for i in range(3):
                state_ref[i, z] = state[i]


def finish_kernel(dims, out_in, part_ref, unit_ref, came_ref, right_ref, out_ref):
    depth, groups, per, lo, space, cores = dims

    @pl.when(lax.axis_index("hi") > 0)
    def _():
        stand = [np.float32(0.5)] * lo
        fields = march(stand, [stand[:1] * 4] * lo, stand, (0.0,) * 3, True)
        added = responses(stand)
        where = {place: k for k, place in enumerate(distinct(lo))}

        def fields_of(j, m):
            k = where[j, m]
            tiles = []
            for z in range(depth * space):
                terms = [] if zero(fields[j][m]) else [part_ref[k, z]]
                for i in range(3):
                    unit = added[i][j][m]
                    if not isinstance(unit, float):
                        unit = unit_ref[i, k, z]
                    terms.append(times(unit, came_ref[i, z]))
                tiles.append(plus(*terms))
            return tiles

        put_fields(dims, fields_of, right_ref, out_ref)


def backward_kernel(dims, got_ref, left_ref, out_hbm, out_ref, sems):
    depth, groups, per = dims[:3]
    width = got_ref.shape[2]
    copies = []
    for i in range(0, 5 * depth, 2):
        pair = jnp.concatenate(
            [
                got_ref[:, k * per : (k + 1) * per, :].reshape(groups * per, width)
                for k in (i, i + 1)
            ],
            axis=1,
        )
        pair = sine_times(pair, left_ref[...])
        for k, plane in ((i, pair[:, :width]), (i + 1, pair[:, width:])):
            out_ref[k] = plane
            copy = pltpu.make_async_copy(
                out_ref.at[k], out_hbm.at[0, k // depth, k % depth], sems.at[k]
            )
            copy.start()
            copies.append(copy)
    for copy in copies:
        copy.wait()


VMEM = pl.BlockSpec(memory_space=pltpu.VMEM)
SMEM = pl.BlockSpec(memory_space=pltpu.SMEM)
HBM = pl.BlockSpec(memory_space=pltpu.HBM)


def call(kernel, shapes, in_specs, scratch=(), out_spec=VMEM, aliases=None):
    return pl.pallas_call(
        kernel,
        out_shape=[jax.ShapeDtypeStruct(s, jnp.float32) for s in shapes],
        in_specs=in_specs,
        out_specs=[out_spec] * len(shapes),
        scratch_shapes=list(scratch),
        input_output_aliases=aliases or {},
        compiler_params=pltpu.CompilerParams(vmem_limit_bytes=12 * 2**20),
    )


def body(initial, start_guess, forcing, step_size):
    depth, width_x, width_y = initial.shape
    hi, lo, chips, cores = (lax.axis_size(a) for a in ("hi", "lo", "chip", "core"))
    space = chips * cores
    groups = space * lo
    per = width_x // groups
    dims = (depth, groups, per, lo, space, cores)
    count = depth * space
    parts = jnp.asarray(sine_parts(width_x))
    right = jnp.asarray(right_table(width_y))
    left = jnp.asarray(left_table(width_x))
    x_weights = jnp.asarray(
        np.broadcast_to(eigen(width_x)[:, None], (width_x, width_y)).astype(np.float32)
    )
    y_weights = jnp.asarray(eigen(width_y)[None, :].astype(np.float32))
    tile = (per, width_y)
    plane = (width_x, width_y)
    bind = functools.partial

    rows = 5 * depth * per
    extra = -(-(per // (lo // depth) + 1) // TILE) * TILE
    blank = pl.pallas_call(
        blank_kernel,
        out_shape=jax.ShapeDtypeStruct((width_x, width_x), parts.dtype),
        out_specs=VMEM,
        cost_estimate=pl.CostEstimate(flops=COST, bytes_accessed=COST, transcendentals=0),
        compiler_params=pltpu.CompilerParams(vmem_limit_bytes=2**20),
    )()
    (send,) = call(
        bind(forward_kernel, dims),
        [(groups, rows + extra, width_y)],
        [SMEM] + [VMEM] * 5,
        [pltpu.VMEM(left.shape, left.dtype)],
    )(step_size, initial, start_guess, forcing, parts, blank)
    members = ("core", "lo", "chip")
    got = lax.all_to_all(send, members, 0, 0, tiled=True)
    state_shape, modes_shape, steps_shape = (3, count, *tile), (lo, 5, count, *tile), (lo, *tile)
    state, modes, steps, start = call(
        bind(first_kernel, dims),
        [state_shape, modes_shape, steps_shape, (count, *tile)],
        [VMEM] * 4,
    )(got, right, x_weights, y_weights)
    onward = [(i, i + lo) for i in range((hi - 1) * lo)]
    onward += [((hi - 1) * lo + i, (i + lo // 2) % lo) for i in range(lo)]
    came = lax.ppermute(state, ("hi", "lo"), onward)
    kinds = len(distinct(lo))
    modes, steps, send, part, unit = call(
        bind(window_kernel, dims),
        [
            modes_shape,
            steps_shape,
            (groups, rows, width_y),
            (kinds, count, *tile),
            (3, kinds, count, *tile),
        ],
        [VMEM] * 7,
        aliases={1: 0, 2: 1},
    )(got, modes, steps, start, right, x_weights, y_weights)
    for _ in range(hi - 2):
        (state,) = call(bind(middle_kernel, dims), [state_shape], [VMEM] * 6, aliases={0: 0})(
            state, modes, steps, came, x_weights, y_weights
        )
        came = lax.ppermute(state, ("hi", "lo"), onward)
    (send,) = call(
        bind(finish_kernel, dims), [(groups, rows, width_y)], [VMEM] * 5, aliases={0: 0}
    )(send, part, unit, came, right)
    got = lax.all_to_all(send, members, 0, 0, tiled=True)
    (fields,) = call(
        bind(backward_kernel, dims),
        [(1, 5, depth, width_x, width_y)],
        [VMEM] * 2,
        [
            pltpu.VMEM((5 * depth, *plane), jnp.float32),
            pltpu.SemaphoreType.DMA((5 * depth,)),
        ],
        HBM,
    )(got, left)
    return fields


def solution(mesh):
    steps, space = mesh.devices.shape
    cores = 2 if space % 2 == 0 else 1
    time, slabs = ("hi", "lo"), ("chip", "core")
    specs = (P(slabs), P(time, slabs), P(time, None, slabs), P(time))

    def run(initial, start_guess, forcing, step_size):
        width = initial.shape[1]
        lo = max(
            d for d in range(1, steps + 1) if steps % d == 0 and width % (TILE * d * space) == 0
        )
        shape = (steps // lo, lo, space // cores, cores)
        whole = Mesh(mesh.devices.reshape(shape), time + slabs)
        return jax.shard_map(
            body, mesh=whole, in_specs=specs, out_specs=P(time, None, slabs), check_vma=False
        )(initial, start_guess, forcing, step_size)

    return run
```

```python
import functools
import math

import jax
import jax.numpy as jnp
import numpy as np
from jax import lax
from jax.experimental import pallas as pl
from jax.experimental.pallas import tpu as pltpu
from jax.sharding import Mesh
from jax.sharding import PartitionSpec as P

TILE = 8
COST = 10**10


def node_tables():
    radical = math.sqrt(3.0 / 7.0)
    node_times = [0.0, (1.0 - radical) / 2.0, 0.5, (1.0 + radical) / 2.0, 1.0]
    integrals = np.zeros((4, 5))
    for column in range(5):
        coeffs = [1.0]
        for other_index in range(5):
            if other_index == column:
                continue
            other_time = node_times[other_index]
            scaling = node_times[column] - other_time
            grown = [0.0] * (len(coeffs) + 1)
            for exponent in range(len(coeffs)):
                grown[exponent + 1] += coeffs[exponent] / scaling
                grown[exponent] -= coeffs[exponent] * other_time / scaling
            coeffs = grown
        for section in range(4):
            integrals[section, column] = sum(
                coeffs[exponent]
                * (node_times[section + 1] ** (exponent + 1) - node_times[section] ** (exponent + 1))
                / (exponent + 1)
                for exponent in range(len(coeffs))
            )
    coarse = [0.0, 0.5, 1.0]
    interp = np.zeros((5, 3))
    for column in range(3):
        for section in range(5):
            weight = 1.0
            for other_index in range(3):
                if other_index != column:
                    weight = (
                        weight
                        * (node_times[section] - coarse[other_index])
                        / (coarse[column] - coarse[other_index])
                    )
            interp[section, column] = weight
    return (np.array(node_times), integrals, interp)


TIMES, QUAD, INTERP = node_tables()
SPACING = np.diff(TIMES)
LEFT = QUAD[0] + QUAD[1]
RIGHT = QUAD[2] + QUAD[3]


def sine(length):
    index = np.arange(1, length + 1)
    return math.sqrt(2.0 / (length + 1)) * np.sin(math.pi / (length + 1) * np.outer(index, index))


def eigen(length):
    return 2.0 - 2.0 * np.cos(math.pi / (length + 1) * np.arange(1, length + 1))


def sine_parts(length):
    matrix = sine(length)
    high = matrix.astype(jnp.bfloat16)
    low = (matrix - high.astype(np.float64)).astype(jnp.bfloat16)
    return np.stack([high, low])


def right_table(length):
    high, low = sine_parts(length)
    return np.block([[high, low], [high, np.zeros_like(high)]])


def left_table(length):
    high, low = sine_parts(length)
    return np.block([[high, high], [low, np.zeros_like(high)]])


def split(value):
    high = value.astype(jnp.bfloat16)
    return high, (value - high.astype(jnp.float32)).astype(jnp.bfloat16)


def times_sine(value, table):
    width = value.shape[-1]
    both = jnp.dot(
        jnp.concatenate(split(value), axis=1), table, preferred_element_type=jnp.float32
    )
    return both[:, :width] + both[:, width:]


def sine_times(value, table):
    width = value.shape[0]
    both = jnp.dot(
        table, jnp.concatenate(split(value), axis=0), preferred_element_type=jnp.float32
    )
    return both[:width] + both[width:]


def sine_list(values):
    count = len(values)
    matrix = sine(count)
    half = count // 2
    even = [values[i] + values[count - 1 - i] for i in range(half)]
    odd = [values[i] - values[count - 1 - i] for i in range(half)]
    middle = [values[half]] if count % 2 else []
    result = []
    for k in range(count):
        terms = even + middle if k % 2 == 0 else odd
        result.append(sum(float(matrix[k, i]) * term for i, term in enumerate(terms)))
    return result


def zero(value):
    return isinstance(value, float) and value == 0.0


def plus(*values):
    values = [v for v in values if not zero(v)]
    return sum(values[1:], values[0]) if values else 0.0


def times(factor, value):
    return 0.0 if zero(factor) or zero(value) else factor * value


def minus(value, other):
    return value if zero(other) else plus(value, -other)


def combine(weights, values):
    merged = {}
    for weight, value in zip(weights, values):
        known = merged.get(id(value), (0.0, value))
        merged[id(value)] = (known[0] + float(weight), value)
    return plus(*(times(w, v) for w, v in merged.values()))


def sweep(first, nodes, forced, scaled):
    unit = np.eye(5)
    swept = [first]
    for m in range(4):
        weights = QUAD[m] - (SPACING[m] * unit[m] if m else 0.0)
        inner = combine(weights, nodes)
        if m:
            inner = plus(inner, times(float(SPACING[m]), swept[m]))
        swept.append(plus(swept[m], times(scaled, inner), forced[m]))
    left = plus(times(scaled, combine(LEFT - 0.5 * unit[0], swept)), *forced[:2])
    right = plus(times(scaled, combine(RIGHT - 0.5 * unit[2], swept)), *forced[2:])
    return swept, left, right


def chain(start, left, right, gain):
    middle = plus(times(gain, start), left)
    return middle, plus(times(gain, middle), right)


def correct(swept, start, middle, ending):
    deltas = [minus(start, swept[0]), minus(middle, swept[2]), minus(ending, swept[4])]
    return [
        start,
        plus(swept[1], combine(INTERP[1], deltas)),
        middle,
        plus(swept[3], combine(INTERP[3], deltas)),
        ending,
    ]


def march(guesses, forced, scaled, state, final):
    before, first, second = state
    fields = []
    for j, guess in enumerate(guesses):
        gain = 1.0 + 0.5 * scaled[j]
        swept, left, right = sweep(before, [before] + [guess] * 4, forced[j], scaled[j])
        middle, ending = chain(first, left, right, gain)
        nodes = correct(swept, first, middle, ending)
        swept, left, right = sweep(first, nodes, forced[j], scaled[j])
        middle, last = chain(second, left, right, gain)
        if final:
            fields.append(correct(swept, second, middle, last))
        before, first, second = guess, ending, last
    return fields if final else (before, first, second)


def responses(scaled):
    nothing = [0.0] * len(scaled)
    return [
        march(nothing, [[0.0] * 4] * len(scaled), scaled, [float(i == k) for k in range(3)], True)
        for i in range(3)
    ]


def distinct(lo):
    return [(j, m) for j in range(lo) for m in range(5) if j == 0 or m]


def blank_kernel(out_ref):
    out_ref[...] = jnp.zeros(out_ref.shape, out_ref.dtype)


def forward_kernel(
    dims, step_ref, init_ref, guess_ref, forcing_ref, parts_ref, blank_ref, out_ref, table_ref
):
    depth, groups, per, lo, space = dims[:5]
    pieces = lo // depth
    width = parts_ref.shape[1]
    high, low = parts_ref[0], parts_ref[1]
    table_ref[:width, :width] = high
    table_ref[:width, width:] = high
    table_ref[width:, :width] = low
    table_ref[width:, width:] = blank_ref[...]

    def transform(planes):
        joined = sine_times(jnp.concatenate(planes, axis=1), table_ref[...])
        half = joined.shape[1] // len(planes)
        return [
            joined[:, i * half : (i + 1) * half].reshape(groups, per, half)
            for i in range(len(planes))
        ]

    def put(field, d, tiles):
        row = (field * depth + d) * per
        out_ref[:, row : row + per, :] = tiles

    starts = transform([init_ref[d] for d in range(depth)])
    mine = lax.axis_index("lo")
    rows = per // pieces
    share = None
    for i in range(lo):
        offset = (i % pieces) * rows
        tile = starts[i // pieces][:, offset : offset + rows]
        share = tile if share is None else jnp.where(mine == i, tile, share)
    step = step_ref[0]
    base = 5 * depth * per
    out_ref[:, base : base + rows, :] = share
    out_ref[:, base + rows :, :] = jnp.full(
        (groups, out_ref.shape[1] - base - rows, out_ref.shape[2]), step, jnp.float32
    )
    for d, tiles in enumerate(transform([guess_ref[0, d] for d in range(depth)])):
        put(0, d, tiles)
    for d in range(depth):
        samples = [forcing_ref[0, j, d] for j in range(5)]
        for m in (0, 2):
            pair = [step * combine(QUAD[k], samples) for k in (m, m + 1)]
            for k, tiles in enumerate(transform(pair)):
                put(1 + m + k, d, tiles)


def source(dims, j, z):
    depth, groups, per, lo, space, cores = dims
    device = z // depth
    return (device % cores * lo + j) * (space // cores) + device // cores, z % depth


def to_modes(dims, got_ref, right_ref, modes_ref, steps_ref):
    depth, groups, per, lo, space, cores = dims
    base = 5 * depth * per + per // (lo // depth)
    count = depth * space
    for j in range(lo):
        columns = []
        for f in range(5):
            tiles = []
            for z in range(count):
                device, d = source(dims, j, z)
                row = (f * depth + d) * per
                tiles.append(got_ref[device, row : row + per, :])
            columns += sine_list(tiles)
        mixed = times_sine(jnp.concatenate(columns, axis=0), right_ref[...])
        modes_ref[j] = mixed.reshape(5, count, per, mixed.shape[1])
        steps_ref[j] = jnp.broadcast_to(
            got_ref[source(dims, j, 0)[0], base : base + 1, :], steps_ref.shape[1:]
        )


def initial_modes(dims, got_ref, right_ref):
    depth, groups, per, lo, space, cores = dims
    pieces = lo // depth
    base = 5 * depth * per
    rows = per // pieces
    tiles = []
    for z in range(depth * space):
        first = (z % depth) * pieces
        parts = [
            got_ref[source(dims, i, z)[0], base : base + rows, :]
            for i in range(first, first + pieces)
        ]
        tiles.append(jnp.concatenate(parts, axis=0))
    mixed = times_sine(jnp.concatenate(sine_list(tiles), axis=0), right_ref[...])
    return mixed.reshape(depth * space, per, mixed.shape[1])


def per_mode(dims, modes_ref, steps_ref, x_ref, y_ref):
    depth, groups, per, lo, space, cores = dims
    device = lax.axis_index("core") * lo + lax.axis_index("lo")
    owner = device * (space // cores) + lax.axis_index("chip")
    plane = x_ref[pl.ds(owner * per, per), :] + y_ref[...]
    steps = [steps_ref[j] for j in range(lo)]
    for z, weight in enumerate(eigen(depth * space)):
        neg = -(plane + float(weight))
        guesses = [modes_ref[j, 0, z] for j in range(lo)]
        forced = [[modes_ref[j, 1 + m, z] for m in range(4)] for j in range(lo)]
        yield z, guesses, forced, [s * neg for s in steps]


def put_fields(dims, fields_of, right_ref, out_ref):
    depth, groups, per, lo, space, cores = dims
    for j in range(lo):
        nodes = range(5) if j == 0 else range(1, 5)
        columns = []
        for m in nodes:
            columns += sine_list(fields_of(j, m))
        mixed = times_sine(jnp.concatenate(columns, axis=0), right_ref[...])
        for k, m in enumerate(nodes):
            places = [(j, m)] + ([(j + 1, 0)] if m == 4 and j + 1 < lo else [])
            for z in range(depth * space):
                first = (k * depth * space + z) * per
                for slot, node in places:
                    device, d = source(dims, slot, z)
                    row = (node * depth + d) * per
                    out_ref[device, row : row + per, :] = mixed[first : first + per]


def first_kernel(
    dims, got_ref, right_ref, x_ref, y_ref, state_ref, modes_ref, steps_ref, start_ref
):
    @pl.when(lax.axis_index("hi") == 0)
    def _():
        to_modes(dims, got_ref, right_ref, modes_ref, steps_ref)
        start_ref[...] = initial_modes(dims, got_ref, right_ref)
        for z, guesses, forced, scaled in per_mode(dims, modes_ref, steps_ref, x_ref, y_ref):
            state = march(guesses, forced, scaled, (start_ref[z],) * 3, False)
            for i in range(3):
                state_ref[i, z] = state[i]


def window_kernel(
    dims, got_ref, modes_in, steps_in, start_ref, right_ref, x_ref, y_ref,
    modes_ref, steps_ref, out_ref, part_ref, unit_ref,
):
    depth, groups, per, lo, space, cores = dims
    head = lax.axis_index("hi") == 0

    @pl.when(head)
    def _():
        for z, guesses, forced, scaled in per_mode(dims, modes_ref, steps_ref, x_ref, y_ref):
            fields = march(guesses, forced, scaled, (start_ref[z],) * 3, True)
            for k, (j, m) in enumerate(distinct(lo)):
                part_ref[k, z] = fields[j][m]
        where = {place: k for k, place in enumerate(distinct(lo))}
        put_fields(
            dims,
            lambda j, m: [part_ref[where[j, m], z] for z in range(depth * space)],
            right_ref,
            out_ref,
        )

    @pl.when(jnp.logical_not(head))
    def _():
        to_modes(dims, got_ref, right_ref, modes_ref, steps_ref)
        for z, guesses, forced, scaled in per_mode(dims, modes_ref, steps_ref, x_ref, y_ref):
            fields = march(guesses, forced, scaled, (0.0,) * 3, True)
            added = responses(scaled)
            for k, (j, m) in enumerate(distinct(lo)):
                if not zero(fields[j][m]):
                    part_ref[k, z] = fields[j][m]
                for i in range(3):
                    if not isinstance(added[i][j][m], float):
                        unit_ref[i, k, z] = added[i][j][m]


def middle_kernel(dims, state_in, modes_ref, steps_ref, came_ref, x_ref, y_ref, state_ref):
    @pl.when(lax.axis_index("hi") > 0)
    def _():
        for z, guesses, forced, scaled in per_mode(dims, modes_ref, steps_ref, x_ref, y_ref):
            came = tuple(came_ref[i, z] for i in range(3))
            state = march(guesses, forced, scaled, came, False)
            for i in range(3):
                state_ref[i, z] = state[i]


def finish_kernel(dims, out_in, part_ref, unit_ref, came_ref, right_ref, out_ref):
    depth, groups, per, lo, space, cores = dims

    @pl.when(lax.axis_index("hi") > 0)
    def _():
        stand = [np.float32(0.5)] * lo
        fields = march(stand, [stand[:1] * 4] * lo, stand, (0.0,) * 3, True)
        added = responses(stand)
        where = {place: k for k, place in enumerate(distinct(lo))}

        def fields_of(j, m):
            k = where[j, m]
            tiles = []
            for z in range(depth * space):
                terms = [] if zero(fields[j][m]) else [part_ref[k, z]]
                for i in range(3):
                    unit = added[i][j][m]
                    if not isinstance(unit, float):
                        unit = unit_ref[i, k, z]
                    terms.append(times(unit, came_ref[i, z]))
                tiles.append(plus(*terms))
            return tiles

        put_fields(dims, fields_of, right_ref, out_ref)


def backward_kernel(dims, got_ref, left_ref, out_hbm, out_ref, sems):
    depth, groups, per = dims[:3]
    width = got_ref.shape[2]
    copies = []
    for i in range(0, 5 * depth, 2):
        pair = jnp.concatenate(
            [
                got_ref[:, k * per : (k + 1) * per, :].reshape(groups * per, width)
                for k in (i, i + 1)
            ],
            axis=1,
        )
        pair = sine_times(pair, left_ref[...])
        for k, plane in ((i, pair[:, :width]), (i + 1, pair[:, width:])):
            out_ref[k] = plane
            copy = pltpu.make_async_copy(
                out_ref.at[k], out_hbm.at[0, k // depth, k % depth], sems.at[k]
            )
            copy.start()
            copies.append(copy)
    for copy in copies:
        copy.wait()


VMEM = pl.BlockSpec(memory_space=pltpu.VMEM)
SMEM = pl.BlockSpec(memory_space=pltpu.SMEM)
HBM = pl.BlockSpec(memory_space=pltpu.HBM)


def call(kernel, shapes, in_specs, scratch=(), out_spec=VMEM, aliases=None):
    return pl.pallas_call(
        kernel,
        out_shape=[jax.ShapeDtypeStruct(s, jnp.float32) for s in shapes],
        in_specs=in_specs,
        out_specs=[out_spec] * len(shapes),
        scratch_shapes=list(scratch),
        input_output_aliases=aliases or {},
        compiler_params=pltpu.CompilerParams(vmem_limit_bytes=12 * 2**20),
    )


def body(initial, start_guess, forcing, step_size):
    depth, width_x, width_y = initial.shape
    hi, lo, chips, cores = (lax.axis_size(a) for a in ("hi", "lo", "chip", "core"))
    space = chips * cores
    groups = space * lo
    per = width_x // groups
    dims = (depth, groups, per, lo, space, cores)
    count = depth * space
    parts = jnp.asarray(sine_parts(width_x))
    right = jnp.asarray(right_table(width_y))
    left = jnp.asarray(left_table(width_x))
    x_weights = jnp.asarray(
        np.broadcast_to(eigen(width_x)[:, None], (width_x, width_y)).astype(np.float32)
    )
    y_weights = jnp.asarray(eigen(width_y)[None, :].astype(np.float32))
    tile = (per, width_y)
    plane = (width_x, width_y)
    bind = functools.partial

    rows = 5 * depth * per
    extra = -(-(per // (lo // depth) + 1) // TILE) * TILE
    blank = pl.pallas_call(
        blank_kernel,
        out_shape=jax.ShapeDtypeStruct((width_x, width_x), parts.dtype),
        out_specs=VMEM,
        cost_estimate=pl.CostEstimate(flops=COST, bytes_accessed=COST, transcendentals=0),
        compiler_params=pltpu.CompilerParams(vmem_limit_bytes=2**20),
    )()
    (send,) = call(
        bind(forward_kernel, dims),
        [(groups, rows + extra, width_y)],
        [SMEM] + [VMEM] * 5,
        [pltpu.VMEM(left.shape, left.dtype)],
    )(step_size, initial, start_guess, forcing, parts, blank)
    members = ("core", "lo", "chip")
    got = lax.all_to_all(send, members, 0, 0, tiled=True)
    state_shape, modes_shape, steps_shape = (3, count, *tile), (lo, 5, count, *tile), (lo, *tile)
    state, modes, steps, start = call(
        bind(first_kernel, dims),
        [state_shape, modes_shape, steps_shape, (count, *tile)],
        [VMEM] * 4,
    )(got, right, x_weights, y_weights)
    onward = [(i, i + lo) for i in range((hi - 1) * lo)]
    onward += [((hi - 1) * lo + i, (i + lo // 2) % lo) for i in range(lo)]
    came = lax.ppermute(state, ("hi", "lo"), onward)
    kinds = len(distinct(lo))
    modes, steps, send, part, unit = call(
        bind(window_kernel, dims),
        [
            modes_shape,
            steps_shape,
            (groups, rows, width_y),
            (kinds, count, *tile),
            (3, kinds, count, *tile),
        ],
        [VMEM] * 7,
        aliases={1: 0, 2: 1},
    )(got, modes, steps, start, right, x_weights, y_weights)
    for _ in range(hi - 2):
        (state,) = call(bind(middle_kernel, dims), [state_shape], [VMEM] * 6, aliases={0: 0})(
            state, modes, steps, came, x_weights, y_weights
        )
        came = lax.ppermute(state, ("hi", "lo"), onward)
    (send,) = call(
        bind(finish_kernel, dims), [(groups, rows, width_y)], [VMEM] * 5, aliases={0: 0}
    )(send, part, unit, came, right)
    got = lax.all_to_all(send, members, 0, 0, tiled=True)
    (fields,) = call(
        bind(backward_kernel, dims),
        [(1, 5, depth, width_x, width_y)],
        [VMEM] * 2,
        [
            pltpu.VMEM((5 * depth, *plane), jnp.float32),
            pltpu.SemaphoreType.DMA((5 * depth,)),
        ],
        HBM,
    )(got, left)
    return fields


def solution(mesh):
    steps, space = mesh.devices.shape
    cores = 2 if space % 2 == 0 else 1
    time, slabs = ("hi", "lo"), ("chip", "core")
    specs = (P(slabs), P(time, slabs), P(time, None, slabs), P(time))

    def run(initial, start_guess, forcing, step_size):
        width = initial.shape[1]
        lo = max(
            d for d in range(1, steps + 1) if steps % d == 0 and width % (TILE * d * space) == 0
        )
        shape = (steps // lo, lo, space // cores, cores)
        whole = Mesh(mesh.devices.reshape(shape), time + slabs)
        return jax.shard_map(
            body, mesh=whole, in_specs=specs, out_specs=P(time, None, slabs), check_vma=False
        )(initial, start_guess, forcing, step_size)

    return run
```

```python
import functools
import math

import jax
import jax.numpy as jnp
import numpy as np
from jax import lax
from jax.experimental import pallas as pl
from jax.experimental.pallas import tpu as pltpu
from jax.sharding import Mesh
from jax.sharding import PartitionSpec as P

TILE = 8
COST = 10**10


def node_tables():
    radical = math.sqrt(3.0 / 7.0)
    node_times = [0.0, (1.0 - radical) / 2.0, 0.5, (1.0 + radical) / 2.0, 1.0]
    integrals = np.zeros((4, 5))
    for column in range(5):
        coeffs = [1.0]
        for other_index in range(5):
            if other_index == column:
                continue
            other_time = node_times[other_index]
            scaling = node_times[column] - other_time
            grown = [0.0] * (len(coeffs) + 1)
            for exponent in range(len(coeffs)):
                grown[exponent + 1] += coeffs[exponent] / scaling
                grown[exponent] -= coeffs[exponent] * other_time / scaling
            coeffs = grown
        for section in range(4):
            integrals[section, column] = sum(
                coeffs[exponent]
                * (node_times[section + 1] ** (exponent + 1) - node_times[section] ** (exponent + 1))
                / (exponent + 1)
                for exponent in range(len(coeffs))
            )
    coarse = [0.0, 0.5, 1.0]
    interp = np.zeros((5, 3))
    for column in range(3):
        for section in range(5):
            weight = 1.0
            for other_index in range(3):
                if other_index != column:
                    weight = (
                        weight
                        * (node_times[section] - coarse[other_index])
                        / (coarse[column] - coarse[other_index])
                    )
            interp[section, column] = weight
    return (np.array(node_times), integrals, interp)


TIMES, QUAD, INTERP = node_tables()
SPACING = np.diff(TIMES)
LEFT = QUAD[0] + QUAD[1]
RIGHT = QUAD[2] + QUAD[3]


def sine(length):
    index = np.arange(1, length + 1)
    return math.sqrt(2.0 / (length + 1)) * np.sin(math.pi / (length + 1) * np.outer(index, index))


def eigen(length):
    return 2.0 - 2.0 * np.cos(math.pi / (length + 1) * np.arange(1, length + 1))


def sine_parts(length):
    matrix = sine(length)
    high = matrix.astype(jnp.bfloat16)
    low = (matrix - high.astype(np.float64)).astype(jnp.bfloat16)
    return np.stack([high, low])


def right_table(length):
    high, low = sine_parts(length)
    return np.block([[high, low], [high, np.zeros_like(high)]])


def left_table(length):
    high, low = sine_parts(length)
    return np.block([[high, high], [low, np.zeros_like(high)]])


def split(value):
    high = value.astype(jnp.bfloat16)
    return high, (value - high.astype(jnp.float32)).astype(jnp.bfloat16)


def times_sine(value, table):
    width = value.shape[-1]
    both = jnp.dot(
        jnp.concatenate(split(value), axis=1), table, preferred_element_type=jnp.float32
    )
    return both[:, :width] + both[:, width:]


def sine_times(value, table):
    width = value.shape[0]
    both = jnp.dot(
        table, jnp.concatenate(split(value), axis=0), preferred_element_type=jnp.float32
    )
    return both[:width] + both[width:]


def sine_list(values):
    count = len(values)
    matrix = sine(count)
    half = count // 2
    even = [values[i] + values[count - 1 - i] for i in range(half)]
    odd = [values[i] - values[count - 1 - i] for i in range(half)]
    middle = [values[half]] if count % 2 else []
    result = []
    for k in range(count):
        terms = even + middle if k % 2 == 0 else odd
        result.append(sum(float(matrix[k, i]) * term for i, term in enumerate(terms)))
    return result


def zero(value):
    return isinstance(value, float) and value == 0.0


def plus(*values):
    values = [v for v in values if not zero(v)]
    return sum(values[1:], values[0]) if values else 0.0


def times(factor, value):
    return 0.0 if zero(factor) or zero(value) else factor * value


def minus(value, other):
    return value if zero(other) else plus(value, -other)


def combine(weights, values):
    merged = {}
    for weight, value in zip(weights, values):
        known = merged.get(id(value), (0.0, value))
        merged[id(value)] = (known[0] + float(weight), value)
    return plus(*(times(w, v) for w, v in merged.values()))


def sweep(first, nodes, forced, scaled):
    unit = np.eye(5)
    swept = [first]
    for m in range(4):
        weights = QUAD[m] - (SPACING[m] * unit[m] if m else 0.0)
        inner = combine(weights, nodes)
        if m:
            inner = plus(inner, times(float(SPACING[m]), swept[m]))
        swept.append(plus(swept[m], times(scaled, inner), forced[m]))
    left = plus(times(scaled, combine(LEFT - 0.5 * unit[0], swept)), *forced[:2])
    right = plus(times(scaled, combine(RIGHT - 0.5 * unit[2], swept)), *forced[2:])
    return swept, left, right


def chain(start, left, right, gain):
    middle = plus(times(gain, start), left)
    return middle, plus(times(gain, middle), right)


def correct(swept, start, middle, ending):
    deltas = [minus(start, swept[0]), minus(middle, swept[2]), minus(ending, swept[4])]
    return [
        start,
        plus(swept[1], combine(INTERP[1], deltas)),
        middle,
        plus(swept[3], combine(INTERP[3], deltas)),
        ending,
    ]


def march(guesses, forced, scaled, state, final):
    before, first, second = state
    fields = []
    for j, guess in enumerate(guesses):
        gain = 1.0 + 0.5 * scaled[j]
        swept, left, right = sweep(before, [before] + [guess] * 4, forced[j], scaled[j])
        middle, ending = chain(first, left, right, gain)
        nodes = correct(swept, first, middle, ending)
        swept, left, right = sweep(first, nodes, forced[j], scaled[j])
        middle, last = chain(second, left, right, gain)
        if final:
            fields.append(correct(swept, second, middle, last))
        before, first, second = guess, ending, last
    return fields if final else (before, first, second)


def responses(scaled):
    nothing = [0.0] * len(scaled)
    return [
        march(nothing, [[0.0] * 4] * len(scaled), scaled, [float(i == k) for k in range(3)], True)
        for i in range(3)
    ]


def distinct(lo):
    return [(j, m) for j in range(lo) for m in range(5) if j == 0 or m]


def blank_kernel(out_ref):
    out_ref[...] = jnp.zeros(out_ref.shape, out_ref.dtype)


def forward_kernel(
    dims, step_ref, init_ref, guess_ref, forcing_ref, parts_ref, blank_ref, out_ref, table_ref
):
    depth, groups, per, lo, space = dims[:5]
    pieces = lo // depth
    width = parts_ref.shape[1]
    high, low = parts_ref[0], parts_ref[1]
    table_ref[:width, :width] = high
    table_ref[:width, width:] = high
    table_ref[width:, :width] = low
    table_ref[width:, width:] = blank_ref[...]

    def transform(planes):
        joined = sine_times(jnp.concatenate(planes, axis=1), table_ref[...])
        half = joined.shape[1] // len(planes)
        return [
            joined[:, i * half : (i + 1) * half].reshape(groups, per, half)
            for i in range(len(planes))
        ]

    def put(field, d, tiles):
        row = (field * depth + d) * per
        out_ref[:, row : row + per, :] = tiles

    starts = transform([init_ref[d] for d in range(depth)])
    mine = lax.axis_index("lo")
    rows = per // pieces
    share = None
    for i in range(lo):
        offset = (i % pieces) * rows
        tile = starts[i // pieces][:, offset : offset + rows]
        share = tile if share is None else jnp.where(mine == i, tile, share)
    step = step_ref[0]
    base = 5 * depth * per
    out_ref[:, base : base + rows, :] = share
    out_ref[:, base + rows :, :] = jnp.full(
        (groups, out_ref.shape[1] - base - rows, out_ref.shape[2]), step, jnp.float32
    )
    for d, tiles in enumerate(transform([guess_ref[0, d] for d in range(depth)])):
        put(0, d, tiles)
    for d in range(depth):
        samples = [forcing_ref[0, j, d] for j in range(5)]
        for m in (0, 2):
            pair = [step * combine(QUAD[k], samples) for k in (m, m + 1)]
            for k, tiles in enumerate(transform(pair)):
                put(1 + m + k, d, tiles)


def source(dims, j, z):
    depth, groups, per, lo, space, cores = dims
    device = z // depth
    return (device % cores * lo + j) * (space // cores) + device // cores, z % depth


def to_modes(dims, got_ref, right_ref, modes_ref, steps_ref, start_ref=None):
    depth, groups, per, lo, space, cores = dims
    base = 5 * depth * per + per // (lo // depth)
    count = depth * space
    columns = []
    for j in range(lo):
        for f in range(5):
            tiles = []
            for z in range(count):
                device, d = source(dims, j, z)
                row = (f * depth + d) * per
                tiles.append(got_ref[device, row : row + per, :])
            columns += sine_list(tiles)
        steps_ref[j] = jnp.broadcast_to(
            got_ref[source(dims, j, 0)[0], base : base + 1, :], steps_ref.shape[1:]
        )
    if start_ref is not None:
        columns += initial_modes(dims, got_ref)
    mixed = times_sine(jnp.concatenate(columns, axis=0), right_ref[...])
    size = 5 * count * per
    for j in range(lo):
        part = mixed[j * size : (j + 1) * size]
        modes_ref[j] = part.reshape(5, count, per, mixed.shape[1])
    if start_ref is not None:
        start_ref[...] = mixed[lo * size :].reshape(count, per, mixed.shape[1])


def initial_modes(dims, got_ref):
    depth, groups, per, lo, space, cores = dims
    pieces = lo // depth
    base = 5 * depth * per
    rows = per // pieces
    tiles = []
    for z in range(depth * space):
        first = (z % depth) * pieces
        parts = [
            got_ref[source(dims, i, z)[0], base : base + rows, :]
            for i in range(first, first + pieces)
        ]
        tiles.append(jnp.concatenate(parts, axis=0))
    return sine_list(tiles)


def per_mode(dims, modes_ref, steps_ref, x_ref, y_ref):
    depth, groups, per, lo, space, cores = dims
    device = lax.axis_index("core") * lo + lax.axis_index("lo")
    owner = device * (space // cores) + lax.axis_index("chip")
    plane = x_ref[pl.ds(owner * per, per), :] + y_ref[...]
    steps = [steps_ref[j] for j in range(lo)]
    for z, weight in enumerate(eigen(depth * space)):
        neg = -(plane + float(weight))
        guesses = [modes_ref[j, 0, z] for j in range(lo)]
        forced = [[modes_ref[j, 1 + m, z] for m in range(4)] for j in range(lo)]
        yield z, guesses, forced, [s * neg for s in steps]


def put_fields(dims, fields_of, right_ref, out_ref):
    depth, groups, per, lo, space, cores = dims
    for j in range(lo):
        nodes = range(5) if j == 0 else range(1, 5)
        columns = []
        for m in nodes:
            columns += sine_list(fields_of(j, m))
        mixed = times_sine(jnp.concatenate(columns, axis=0), right_ref[...])
        for k, m in enumerate(nodes):
            places = [(j, m)] + ([(j + 1, 0)] if m == 4 and j + 1 < lo else [])
            for z in range(depth * space):
                first = (k * depth * space + z) * per
                for slot, node in places:
                    device, d = source(dims, slot, z)
                    row = (node * depth + d) * per
                    out_ref[device, row : row + per, :] = mixed[first : first + per]


def first_kernel(
    dims, got_ref, right_ref, x_ref, y_ref, state_ref, modes_ref, steps_ref, start_ref
):
    @pl.when(lax.axis_index("hi") == 0)
    def _():
        to_modes(dims, got_ref, right_ref, modes_ref, steps_ref, start_ref)
        for z, guesses, forced, scaled in per_mode(dims, modes_ref, steps_ref, x_ref, y_ref):
            state = march(guesses, forced, scaled, (start_ref[z],) * 3, False)
            for i in range(3):
                state_ref[i, z] = state[i]


def window_kernel(
    dims, got_ref, modes_in, steps_in, start_ref, right_ref, x_ref, y_ref,
    modes_ref, steps_ref, out_ref, part_ref, unit_ref,
):
    depth, groups, per, lo, space, cores = dims
    head = lax.axis_index("hi") == 0

    @pl.when(head)
    def _():
        for z, guesses, forced, scaled in per_mode(dims, modes_ref, steps_ref, x_ref, y_ref):
            fields = march(guesses, forced, scaled, (start_ref[z],) * 3, True)
            for k, (j, m) in enumerate(distinct(lo)):
                part_ref[k, z] = fields[j][m]
        where = {place: k for k, place in enumerate(distinct(lo))}
        put_fields(
            dims,
            lambda j, m: [part_ref[where[j, m], z] for z in range(depth * space)],
            right_ref,
            out_ref,
        )

    @pl.when(jnp.logical_not(head))
    def _():
        to_modes(dims, got_ref, right_ref, modes_ref, steps_ref)
        for z, guesses, forced, scaled in per_mode(dims, modes_ref, steps_ref, x_ref, y_ref):
            fields = march(guesses, forced, scaled, (0.0,) * 3, True)
            added = responses(scaled)
            for k, (j, m) in enumerate(distinct(lo)):
                if not zero(fields[j][m]):
                    part_ref[k, z] = fields[j][m]
                for i in range(3):
                    if not isinstance(added[i][j][m], float):
                        unit_ref[i, k, z] = added[i][j][m]


def middle_kernel(dims, state_in, modes_ref, steps_ref, came_ref, x_ref, y_ref, state_ref):
    @pl.when(lax.axis_index("hi") > 0)
    def _():
        for z, guesses, forced, scaled in per_mode(dims, modes_ref, steps_ref, x_ref, y_ref):
            came = tuple(came_ref[i, z] for i in range(3))
            state = march(guesses, forced, scaled, came, False)
            for i in range(3):
                state_ref[i, z] = state[i]


def finish_kernel(dims, out_in, part_ref, unit_ref, came_ref, right_ref, out_ref):
    depth, groups, per, lo, space, cores = dims

    @pl.when(lax.axis_index("hi") > 0)
    def _():
        stand = [np.float32(0.5)] * lo
        fields = march(stand, [stand[:1] * 4] * lo, stand, (0.0,) * 3, True)
        added = responses(stand)
        where = {place: k for k, place in enumerate(distinct(lo))}

        def fields_of(j, m):
            k = where[j, m]
            tiles = []
            for z in range(depth * space):
                terms = [] if zero(fields[j][m]) else [part_ref[k, z]]
                for i in range(3):
                    unit = added[i][j][m]
                    if not isinstance(unit, float):
                        unit = unit_ref[i, k, z]
                    terms.append(times(unit, came_ref[i, z]))
                tiles.append(plus(*terms))
            return tiles

        put_fields(dims, fields_of, right_ref, out_ref)


def backward_kernel(dims, got_ref, left_ref, out_hbm, out_ref, sems):
    depth, groups, per = dims[:3]
    width = got_ref.shape[2]
    copies = []
    for i in range(0, 5 * depth, 2):
        pair = jnp.concatenate(
            [
                got_ref[:, k * per : (k + 1) * per, :].reshape(groups * per, width)
                for k in (i, i + 1)
            ],
            axis=1,
        )
        pair = sine_times(pair, left_ref[...])
        for k, plane in ((i, pair[:, :width]), (i + 1, pair[:, width:])):
            out_ref[k] = plane
            copy = pltpu.make_async_copy(
                out_ref.at[k], out_hbm.at[0, k // depth, k % depth], sems.at[k]
            )
            copy.start()
            copies.append(copy)
    for copy in copies:
        copy.wait()


VMEM = pl.BlockSpec(memory_space=pltpu.VMEM)
SMEM = pl.BlockSpec(memory_space=pltpu.SMEM)
HBM = pl.BlockSpec(memory_space=pltpu.HBM)


def call(kernel, shapes, in_specs, scratch=(), out_spec=VMEM, aliases=None):
    return pl.pallas_call(
        kernel,
        out_shape=[jax.ShapeDtypeStruct(s, jnp.float32) for s in shapes],
        in_specs=in_specs,
        out_specs=[out_spec] * len(shapes),
        scratch_shapes=list(scratch),
        input_output_aliases=aliases or {},
        compiler_params=pltpu.CompilerParams(vmem_limit_bytes=12 * 2**20),
    )


def body(initial, start_guess, forcing, step_size):
    depth, width_x, width_y = initial.shape
    hi, lo, chips, cores = (lax.axis_size(a) for a in ("hi", "lo", "chip", "core"))
    space = chips * cores
    groups = space * lo
    per = width_x // groups
    dims = (depth, groups, per, lo, space, cores)
    count = depth * space
    parts = jnp.asarray(sine_parts(width_x))
    right = jnp.asarray(right_table(width_y))
    left = jnp.asarray(left_table(width_x))
    x_weights = jnp.asarray(
        np.broadcast_to(eigen(width_x)[:, None], (width_x, width_y)).astype(np.float32)
    )
    y_weights = jnp.asarray(eigen(width_y)[None, :].astype(np.float32))
    tile = (per, width_y)
    plane = (width_x, width_y)
    bind = functools.partial

    rows = 5 * depth * per
    extra = -(-(per // (lo // depth) + 1) // TILE) * TILE
    blank = pl.pallas_call(
        blank_kernel,
        out_shape=jax.ShapeDtypeStruct((width_x, width_x), parts.dtype),
        out_specs=VMEM,
        cost_estimate=pl.CostEstimate(flops=COST, bytes_accessed=COST, transcendentals=0),
        compiler_params=pltpu.CompilerParams(vmem_limit_bytes=2**20),
    )()
    (send,) = call(
        bind(forward_kernel, dims),
        [(groups, rows + extra, width_y)],
        [SMEM] + [VMEM] * 5,
        [pltpu.VMEM(left.shape, left.dtype)],
    )(step_size, initial, start_guess, forcing, parts, blank)
    members = ("core", "lo", "chip")
    got = lax.all_to_all(send, members, 0, 0, tiled=True)
    state_shape, modes_shape, steps_shape = (3, count, *tile), (lo, 5, count, *tile), (lo, *tile)
    state, modes, steps, start = call(
        bind(first_kernel, dims),
        [state_shape, modes_shape, steps_shape, (count, *tile)],
        [VMEM] * 4,
    )(got, right, x_weights, y_weights)
    onward = [(i, i + lo) for i in range((hi - 1) * lo)]
    onward += [((hi - 1) * lo + i, (i + lo // 2) % lo) for i in range(lo)]
    came = lax.ppermute(state, ("hi", "lo"), onward)
    kinds = len(distinct(lo))
    modes, steps, send, part, unit = call(
        bind(window_kernel, dims),
        [
            modes_shape,
            steps_shape,
            (groups, rows, width_y),
            (kinds, count, *tile),
            (3, kinds, count, *tile),
        ],
        [VMEM] * 7,
        aliases={1: 0, 2: 1},
    )(got, modes, steps, start, right, x_weights, y_weights)
    for _ in range(hi - 2):
        (state,) = call(bind(middle_kernel, dims), [state_shape], [VMEM] * 6, aliases={0: 0})(
            state, modes, steps, came, x_weights, y_weights
        )
        came = lax.ppermute(state, ("hi", "lo"), onward)
    (send,) = call(
        bind(finish_kernel, dims), [(groups, rows, width_y)], [VMEM] * 5, aliases={0: 0}
    )(send, part, unit, came, right)
    got = lax.all_to_all(send, members, 0, 0, tiled=True)
    (fields,) = call(
        bind(backward_kernel, dims),
        [(1, 5, depth, width_x, width_y)],
        [VMEM] * 2,
        [
            pltpu.VMEM((5 * depth, *plane), jnp.float32),
            pltpu.SemaphoreType.DMA((5 * depth,)),
        ],
        HBM,
    )(got, left)
    return fields


def solution(mesh):
    steps, space = mesh.devices.shape
    cores = 2 if space % 2 == 0 else 1
    time, slabs = ("hi", "lo"), ("chip", "core")
    specs = (P(slabs), P(time, slabs), P(time, None, slabs), P(time))

    def run(initial, start_guess, forcing, step_size):
        width = initial.shape[1]
        lo = max(
            d for d in range(1, steps + 1) if steps % d == 0 and width % (TILE * d * space) == 0
        )
        shape = (steps // lo, lo, space // cores, cores)
        whole = Mesh(mesh.devices.reshape(shape), time + slabs)
        return jax.shard_map(
            body, mesh=whole, in_specs=specs, out_specs=P(time, None, slabs), check_vma=False
        )(initial, start_guess, forcing, step_size)

    return run
```
